256 devices in a mesh: grp: 4 (over x), dev: 64 (over z, y, core).
Axes of the slice: x: 4, y: 4, z: 8, core: 2. Of those that a mesh axis runs over, the one named last changes fastest.
Arguments:
- block_values: bfloat16 [3072, 9, 128, 128], P(('grp', 'dev')), may hold values from -0.1875 to 0.1875
- block_columns: int32 [3072, 9], P(('grp', 'dev')), may hold values from 0 to 17, as said below
- tentative: bfloat16 [3072, 128, 128], P(('grp', 'dev')), may hold values from -1.1953125 to 1.1953125
- inverse_diagonal: bfloat16 [3072, 128, 128], P(('grp', 'dev')), may hold values from -0.5 to 0.5
- aggregate: int32 [3072], P(('grp', 'dev')), may hold values from 0 to 1, as said below
- ghost_rows: int32 [256, 2, 3], P(('grp', 'dev')), may hold values from 0 to 11, as said below
- damping: float32 [1], replicated, may hold values from 0.5 to 0.8
Outputs:
- coarse_op: bfloat16 [512, 128, 1792], P(('grp', 'dev'))
The draws below stay inside these ranges and needn't reach their ends.
Inputs may be any that keep to these rules, and one draw needn't show every extreme that they name: `block_columns`: in part n, row r names its own row r first; the 9 entries of a row differ; entries from 12 to 14 never stand in the first part, entries from 15 on never in the last. `aggregate`: each of the 2 aggregates of a part holds one or more of its rows. `ghost_rows`: the 3 rows of each list differ.
All inputs are finite; a program needn't handle non-finite values.
Results may differ from the reference program's by a relative error of at most 0.0068.
Values may be sent and summed in bfloat16 or wider, within the bound.
No kernel may reach another device: no remote copies, remote signals or barrier semaphores. Data moves between devices by JAX's collectives and lax.ppermute only.
A program may use at most 64 MiB of HBM per device.

```python
import jax
import jax.numpy as jnp
from jax import lax

B = 128
K = 9
CA = 2
R = 12
S = 3
NB = 3072
N_GRP = 4
N_DEV = 64


def draw_block_columns(key, part):
    key = jax.random.fold_in(key, 11)
    devices = N_GRP * N_DEV
    choices_all = R + 2 * S
    candidate = jnp.arange(choices_all, dtype=jnp.int32)[None, None, :]
    device_index = jnp.arange(devices, dtype=jnp.int32)[:, None, None]
    row_index = jnp.arange(R, dtype=jnp.int32)[None, :, None]
    left_ghost = (candidate >= R) & (candidate < R + S)
    right_ghost = candidate >= R + S
    usable = (candidate != row_index) & ~(left_ghost & (device_index == 0)) & ~(right_ghost & (device_index == devices - 1))
    scores = jax.random.randint(key, (devices, R, choices_all), 0, 1 << 20) * choices_all + candidate
    scores = jnp.where(usable, scores, -1)
    picked = lax.top_k(scores, K - 1)[0] % choices_all
    first = jnp.broadcast_to(row_index, (devices, R, 1))
    return jnp.concatenate([first, picked], axis=2).reshape(devices * R, K).astype(jnp.int32)


def draw_aggregate(key, part):
    devices = N_GRP * N_DEV
    keys_all = jax.random.split(jax.random.fold_in(key, 23), devices)
    orders = jax.vmap(lambda single: jax.random.permutation(single, R))(keys_all)
    extra = jax.random.randint(jax.random.fold_in(key, 24), (devices, R), 0, CA)
    position = jnp.arange(R, dtype=jnp.int32)[None, :]
    labels = jnp.where(position < CA, position, extra)
    inverse = jnp.argsort(orders, axis=1)
    return jnp.take_along_axis(labels, inverse, axis=1).reshape(devices * R).astype(jnp.int32)


def draw_ghost_rows(key, part):
    devices = N_GRP * N_DEV
    keys_all = jax.random.split(jax.random.fold_in(key, 37), devices * 2)
    orders = jax.vmap(lambda single: jax.random.permutation(single, R))(keys_all)
    return orders[:, :S].reshape(devices, 2, S).astype(jnp.int32)


def shard_levels(key, shape, cuts, least, top_value):
    def one(axis_at, shards_of):
        steps = jax.random.uniform(jax.random.fold_in(jax.random.fold_in(key, 6), axis_at), (shards_of,), jnp.float32, least / len(cuts), top_value / len(cuts))
        return jnp.repeat(jnp.exp(steps), shape[axis_at] // shards_of).reshape((-1,) + (1,) * (len(shape) - axis_at - 1))

    factor_of = one(*cuts[0])
    for cut in cuts[1:]:
        factor_of = factor_of * one(*cut)
    return factor_of


def normal_values(own_key, dims, scale, limit, cuts=(), kind=jnp.bfloat16):
    entries = scale * jax.random.normal(own_key, dims, jnp.float32)
    if cuts:
        entries = entries * shard_levels(own_key, dims, cuts, -0.22, 0.18)
    return jnp.clip(entries, -limit, limit).astype(kind)


def setup_inputs(seed: int = 0) -> dict:
    splits = jax.random.split(jax.random.key(seed), 8)
    return {
        "block_values": normal_values(splits[0], (NB, K, B, B), (K * B) ** -0.5, 0.1875, ((0, 256),)),
        "block_columns": draw_block_columns(jax.random.fold_in(splits[7], 71), 0),
        "tentative": normal_values(splits[2], (NB, B, B), 0.2, 1.1953125, ((0, 256),)),
        "inverse_diagonal": normal_values(splits[3], (NB, B, B), B ** -0.5, 0.5, ((0, 256),)),
        "aggregate": draw_aggregate(jax.random.fold_in(splits[7], 71), 0),
        "ghost_rows": draw_ghost_rows(jax.random.fold_in(splits[7], 71), 0),
        "damping": jnp.clip(jax.random.uniform(splits[6], (1,), jnp.float32, 0.5, 0.8), 0.5, 0.8),
    }


def place_own(tentative, aggregate):
    aggregate_mask = aggregate[:, None] == jnp.arange(CA, dtype=jnp.int32)[None, :]
    spread = jnp.where(aggregate_mask[:, None, :, None], tentative[:, :, None, :], jnp.zeros((), tentative.dtype))
    return spread.reshape(tentative.shape[0], tentative.shape[1], CA * tentative.shape[2])


def side_of(columns):
    return jnp.where(columns < R, 1, jnp.where(columns < R + S, 0, 2)).astype(jnp.int32)


def by_side(product_term, column_side, block_span):
    left_pad = jnp.pad(product_term, ((0, 0), (0, 0), (0, 2 * block_span)))
    middle_pad = jnp.pad(product_term, ((0, 0), (0, 0), (block_span, block_span)))
    right_pad = jnp.pad(product_term, ((0, 0), (0, 0), (2 * block_span, 0)))
    side_index = column_side[:, None, None]
    return jnp.where(side_index == 0, left_pad, jnp.where(side_index == 1, middle_pad, right_pad))


def assemble(values, columns, column_side, lookup, block_span):
    start = jnp.zeros((values.shape[0], B, lookup.shape[2] + 2 * block_span), jnp.float32)

    def accumulate(slot_index, running_sum):
        column_now = lax.dynamic_index_in_dim(columns, slot_index, 1, keepdims=False)
        side_now = lax.dynamic_index_in_dim(column_side, slot_index, 1, keepdims=False)
        value_now = lax.dynamic_index_in_dim(values, slot_index, 1, keepdims=False)
        picked = jnp.take(lookup, column_now, axis=0)
        product_term = jnp.einsum("rab,rbc->rac", value_now.astype(jnp.float32), picked.astype(jnp.float32), precision=lax.Precision.HIGHEST)
        return running_sum + by_side(product_term, side_now, block_span)

    return lax.fori_loop(0, values.shape[1], accumulate, start)


def neighbours(shards):
    blank = jnp.zeros_like(shards[:1])
    return jnp.concatenate([blank, shards[:-1]], axis=0), jnp.concatenate([shards[1:], blank], axis=0)


def reference(block_values, block_columns, tentative, inverse_diagonal, aggregate, ghost_rows, damping):
    devices = N_GRP * N_DEV
    block_span = CA * B
    own_all = place_own(tentative, aggregate).reshape(devices, R, B, block_span)
    values_all = block_values.reshape(devices, R, K, B, B)
    columns_all = block_columns.reshape(devices, R, K)
    inverse_all = inverse_diagonal.reshape(devices, R, B, B)
    left_all, right_all = neighbours(own_all)

    def smooth_part(pieces):
        values, columns, ghost_lists, own_rows, left_rows, right_rows, inverse = pieces
        column_side = side_of(columns)
        lookup = jnp.concatenate([own_rows, jnp.take(left_rows, ghost_lists[0], axis=0), jnp.take(right_rows, ghost_lists[1], axis=0)], axis=0)
        smooth_sum = assemble(values, columns, column_side, lookup, block_span)
        smooth_half = lax.optimization_barrier(smooth_sum.astype(jnp.bfloat16))
        scaled = jnp.einsum("rab,rbc->rac", inverse.astype(jnp.float32), smooth_half.astype(jnp.float32), precision=lax.Precision.HIGHEST)
        own_wide = jnp.pad(own_rows, ((0, 0), (0, 0), (block_span, block_span))).astype(jnp.float32)
        return (own_wide - damping[0] * scaled).astype(jnp.bfloat16)

    prolong_all = lax.map(smooth_part, (values_all, columns_all, ghost_rows, own_all, left_all, right_all, inverse_all))
    left_prolong, right_prolong = neighbours(prolong_all)

    def galerkin_part(pieces):
        values, columns, ghost_lists, own_rows, left_rows, right_rows = pieces
        column_side = side_of(columns)
        lookup = jnp.concatenate([own_rows, jnp.take(left_rows, ghost_lists[0], axis=0), jnp.take(right_rows, ghost_lists[1], axis=0)], axis=0)
        applied = assemble(values, columns, column_side, lookup, block_span).astype(jnp.bfloat16)
        flat_prolong = own_rows.reshape(R * B, 3 * block_span).astype(jnp.float32)
        flat_applied = applied.reshape(R * B, 5 * block_span).astype(jnp.float32)
        return lax.dot_general(flat_prolong, flat_applied, (((0,), (0,)), ((), ())), precision=lax.Precision.HIGHEST)

    partial_rows = lax.map(galerkin_part, (values_all, columns_all, ghost_rows, prolong_all, left_prolong, right_prolong))
    blank = jnp.zeros_like(partial_rows[:1, :block_span])
    middle = partial_rows[:, block_span:2 * block_span]
    from_right = jnp.concatenate([partial_rows[1:, :block_span], blank], axis=0)
    from_left = jnp.concatenate([blank, partial_rows[:-1, 2 * block_span:]], axis=0)
    coarse = jnp.pad(middle, ((0, 0), (0, 0), (block_span, block_span)))
    coarse = coarse + jnp.pad(from_right, ((0, 0), (0, 0), (2 * block_span, 0)))
    coarse = coarse + jnp.pad(from_left, ((0, 0), (0, 0), (0, 2 * block_span)))
    return coarse.reshape(devices * CA, B, 7 * block_span).astype(jnp.bfloat16)
```

```python
import functools

import jax
import jax.numpy as jnp
from jax import lax
from jax.experimental import pallas as pl
from jax.experimental.pallas import tpu as pltpu
from jax.sharding import PartitionSpec as P

CA = 2
META = 32
AXES = ("grp", "dev")
VMEM = pltpu.VMEM
SMEM = pltpu.SMEM
F32 = jnp.float32
BF16 = jnp.bfloat16


SPACES = {"v": VMEM, "s": SMEM, "h": pltpu.HBM}


def call(kernel, args, spaces, outs, scratch=(), flops=1, limit=None):
    nbytes = sum(a.size * a.dtype.itemsize for a in args)
    in_specs = [pl.BlockSpec(memory_space=SPACES[c]) for c in spaces]
    return pl.pallas_call(
        kernel,
        out_shape=[jax.ShapeDtypeStruct(*o) for o in outs],
        in_specs=in_specs,
        out_specs=[pl.BlockSpec(memory_space=VMEM) for _ in outs],
        scratch_shapes=list(scratch),
        cost_estimate=pl.CostEstimate(flops=flops, bytes_accessed=nbytes, transcendentals=0),
        compiler_params=pltpu.CompilerParams(vmem_limit_bytes=limit),
    )(*[pltpu.with_memory_space_constraint(a, pltpu.HBM) if c == "h" else a for a, c in zip(args, spaces)])


def rows(index, size):
    return pl.ds(pl.multiple_of(index * size, size), size)


def dot(a, b):
    return jnp.dot(a, b, preferred_element_type=F32)


def pack_kernel(r, b, s, agg_hbm, ghost_hbm, tent_hbm, out, agg, ghost, sems):
    copies = [
        pltpu.make_async_copy(agg_hbm, agg, sems.at[0]),
        pltpu.make_async_copy(ghost_hbm, ghost, sems.at[1]),
        pltpu.make_async_copy(tent_hbm, out.at[: r * b, :], sems.at[2]),
    ]
    for copy in copies:
        copy.start()
    copies[0].wait()
    copies[1].wait()
    sub = lax.broadcasted_iota(jnp.int32, (META, b), 0)
    meta = jnp.zeros((META, b), F32)
    for j in range(r):
        meta = jnp.where(sub == j, agg[j].astype(F32), meta)
    for side in range(2):
        for j in range(s):
            meta = jnp.where(sub == 16 + 8 * side + j, ghost[0, side, j].astype(F32), meta)
    out[r * b :, :] = meta.astype(BF16)
    copies[2].wait()


def own_kernel(
    r, k, b, s, cols_hbm, agg_hbm, par, damp, vals_hbm, inv_hbm, pay, dense, inv, p_own, cols, agg, vals, placed, sems
):
    def fetch(j):
        return pltpu.make_async_copy(vals_hbm.at[j], vals.at[j], sems.at[j])

    others = [
        pltpu.make_async_copy(cols_hbm, cols, sems.at[r]),
        pltpu.make_async_copy(agg_hbm, agg, sems.at[r + 1]),
        pltpu.make_async_copy(inv_hbm, inv, sems.at[r + 2]),
    ]
    others[0].start()
    others[1].start()
    for j in range(r):
        fetch(j).start()
    others[2].start()

    def clear(j, carry):
        dense[rows(j, b), :] = jnp.zeros((b, (r + 2 * s) * b), BF16)
        return carry

    lax.fori_loop(0, r, clear, 0)
    others[0].wait()
    others[1].wait()
    zero = jnp.zeros((b, b), BF16)
    for j in range(r):
        own = slice(j * b, (j + 1) * b)
        block = pay[own, :]
        here = agg[j]
        for c in range(CA):
            placed[own, c * b : (c + 1) * b] = jnp.where(here == c, block, zero)
    odd = par[0]
    left = s * (1 - odd)

    def row(j, carry):
        fetch(j).wait()
        at = rows(j, b)
        for e in range(k):
            c = cols[j, e]
            c = jnp.where(c < r, c, jnp.where(c < r + s, c + left, c - left))
            dense[at, rows(c, b)] = vals[j, e]
        return carry

    lax.fori_loop(0, r, row, 0)
    others[2].wait()
    step = 4

    def smooth(t, carry):
        half = dot(dense[rows(t, step * b), : r * b], placed[...]).astype(BF16)
        for q in range(step):
            at = rows(t * step + q, b)
            scaled = dot(inv[at, :], half[q * b : (q + 1) * b, :])
            p_own[at, :] = (placed[at, :].astype(F32) - damp[0] * scaled).astype(BF16)
        return carry

    lax.fori_loop(0, r // step, smooth, 0)


def ghost_kernel(r, b, s, ghost, par, damp, dense, inv, p_own, pay_s, pay_x, p_s, p_x, out_s, out_x, meta, placed):
    odd = par[0]
    sides = ((pay_s, 1 - odd, odd), (pay_x, odd, 1 - odd))
    for d, (pay, mine, _) in enumerate(sides):
        meta[d] = pay[r * b :, :].astype(F32)
        for j in range(s):
            row = jnp.clip(ghost[0, mine, j], 0, r - 1)
            block = pay[rows(row, b), :]
            here = jnp.broadcast_to(meta[d, pl.ds(row, 1), :], (b, b))
            at = slice((d * s + j) * b, (d * s + j + 1) * b)
            for c in range(CA):
                placed[at, c * b : (c + 1) * b] = jnp.where(here == c, block.astype(F32), 0.0).astype(BF16)
    step = 4
    for d, target in enumerate((p_s, p_x)):
        span = slice(d * s * b, (d + 1) * s * b)
        cols = slice((r + d * s) * b, (r + d * s + s) * b)

        def smooth(t, carry):
            half = dot(dense[rows(t, step * b), cols], placed[span, :]).astype(BF16)
            for q in range(step):
                at = rows(t * step + q, b)
                scaled = dot(inv[at, :], half[q * b : (q + 1) * b, :])
                target[at, :] = (-damp[0] * scaled).astype(BF16)
            return carry

        lax.fori_loop(0, r // step, smooth, 0)
    w = CA * b
    for d, (_, mine, theirs) in enumerate(sides):
        out = (out_s, out_x)[d]
        for j in range(s):
            wanted = meta[d, pl.ds(16 + 8 * theirs + j, 1), :]
            row = jnp.clip(jnp.max(wanted).astype(jnp.int32), 0, r - 1)
            at = rows(row, b)
            to = slice(j * b, (j + 1) * b)
            out[to, :w] = p_s[at, :]
            out[to, w : 2 * w] = p_own[at, :]
            out[to, 2 * w :] = p_x[at, :]


def middle_kernel(r, b, w, dense, p_s, p_own, p_x, gal, wide, flipped, applied):
    parts = (p_s, p_own, p_x)
    for d, p in enumerate(parts):
        for j in range(r):
            at = slice(j * b, (j + 1) * b)
            flipped[d * w : (d + 1) * w, at] = p[at, :].T
    step = 4

    def apply(t, carry):
        at = rows(t, step * b)
        block = dense[at, : r * b]
        for d, p in enumerate(parts):
            applied[at, d * w : (d + 1) * w] = dot(block, p[...]).astype(BF16)
        return carry

    lax.fori_loop(0, r // step, apply, 0)

    def galerkin(t, carry):
        at = rows(t, w)
        left = flipped[at, :]
        gal[at, :] = dot(left, applied[...])
        wide[at, :] = dot(left, dense[:, r * b :]).astype(BF16)
        return carry

    lax.fori_loop(0, 3, galerkin, 0)


def galerkin_rows(index, w, span, gal, wide, far_s, far_x, write):
    at = slice(index * w, (index + 1) * w)
    left_s = wide[at, :span]
    left_x = wide[at, span:]
    by_s = dot(left_s, far_s[...])
    by_x = dot(left_x, far_x[...])
    write(0, by_s[:, 2 * w :])
    write(1, gal[at, :w] + by_s[:, w : 2 * w])
    write(2, gal[at, w : 2 * w] + by_s[:, :w] + by_x[:, 2 * w :])
    write(3, gal[at, 2 * w :] + by_x[:, w : 2 * w])
    write(4, by_x[:, :w])


def outer_kernel(w, span, gal, wide, far_s, far_x, out_x, out_s):
    for index, out in ((2, out_x), (0, out_s)):
        def write(c, value, out=out):
            out[:, c * w : (c + 1) * w] = value.astype(BF16)

        galerkin_rows(index, w, span, gal, wide, far_s, far_x, write)


def inner_kernel(w, span, gal, wide, far_s, far_x, out):
    def write(c, value):
        out[:, c * w : (c + 1) * w] = value

    galerkin_rows(1, w, span, gal, wide, far_s, far_x, write)


def final_kernel(w, par, mine, from_s, from_x, out):
    sign = 1 - 2 * par[0]
    for u in range(-3, 4):
        total = None
        for ref, at in ((mine, 2 - u), (from_s, 1 + u), (from_x, 3 + u)):
            if 0 <= at < 5:
                term = ref[:, at * w : (at + 1) * w].astype(F32)
                total = term if total is None else total + term
        out[:, rows(3 + sign * u, w)] = total.astype(BF16)


def swap(x, route):
    return lax.ppermute(x, AXES, route)


def shards(block_values, block_columns, tentative, inverse_diagonal, aggregate, ghost_rows, damping):
    r, k = block_columns.shape
    b = tentative.shape[1]
    s = ghost_rows.shape[2]
    w = CA * b
    span = s * b
    devices = lax.axis_size(AXES)
    chip = [(i, i ^ 1) for i in range(devices) if i ^ 1 < devices]
    cross = []
    for i in range(1, devices - 1, 2):
        cross += [(i, i + 1), (i + 1, i)]
    par = (lax.axis_index(AXES) % 2).astype(jnp.int32).reshape(1)
    tent = tentative.reshape(r * b, b)
    inv = inverse_diagonal.reshape(r * b, b)
    dma = pltpu.SemaphoreType.DMA

    (pay,) = call(
        functools.partial(pack_kernel, r, b, s), (aggregate, ghost_rows, tent), "hhh",
        [((r * b + META, b), BF16)],
        scratch=[SMEM((r,), jnp.int32), SMEM((1, 2, s), jnp.int32), dma((3,))], limit=2 << 20,
    )
    pay_x = swap(pay, cross)
    pay_s = swap(pay, chip)
    dense, inv, p_own = call(
        functools.partial(own_kernel, r, k, b, s),
        (block_columns, aggregate, par, damping, block_values, inv, pay), "hhsshhv",
        [((r * b, (r + 2 * s) * b), BF16), ((r * b, b), BF16), ((r * b, w), BF16)],
        scratch=[
            SMEM((r, k), jnp.int32), SMEM((r,), jnp.int32), VMEM((r, k, b, b), BF16), VMEM((r * b, w), BF16),
            dma((r + 3,)),
        ],
        flops=2 * r * b * r * b * w, limit=24 << 20,
    )
    p_s, p_x, out_s, out_x = call(
        functools.partial(ghost_kernel, r, b, s),
        (ghost_rows, par, damping, dense, inv, p_own, pay_s, pay_x), "sssvvvvv",
        [((r * b, w), BF16), ((r * b, w), BF16), ((span, 3 * w), BF16), ((span, 3 * w), BF16)],
        scratch=[VMEM((2, META, b), F32), VMEM((2 * span, w), BF16)],
        flops=2 * r * b * 2 * span * w, limit=24 << 20,
    )
    far_x = swap(out_x, cross)
    far_s = swap(out_s, chip)
    gal, wide = call(
        functools.partial(middle_kernel, r, b, w), (dense, p_s, p_own, p_x), "vvvv",
        [((3 * w, 3 * w), F32), ((3 * w, 2 * span), BF16)],
        scratch=[VMEM((3 * w, r * b), BF16), VMEM((r * b, 3 * w), BF16)],
        flops=6 * r * b * r * b * w, limit=24 << 20,
    )
    sum_x, sum_s = call(
        functools.partial(outer_kernel, w, span), (gal, wide, far_s, far_x), "vvvv",
        [((w, 5 * w), BF16), ((w, 5 * w), BF16)], flops=8 * w * span * 3 * w, limit=16 << 20,
    )
    from_x = swap(sum_x, cross)
    from_s = swap(sum_s, chip)
    (mine,) = call(
        functools.partial(inner_kernel, w, span), (gal, wide, far_s, far_x), "vvvv",
        [((w, 5 * w), F32)], flops=4 * w * span * 3 * w, limit=16 << 20,
    )
    (out,) = call(
        functools.partial(final_kernel, w), (par, mine, from_s, from_x), "svvv",
        [((w, 7 * w), BF16)], flops=w * 7 * w, limit=16 << 20,
    )
    return out.reshape(CA, b, 7 * w)


def solution(mesh):
    return jax.shard_map(
        shards,
        mesh=mesh,
        in_specs=(
            P(AXES, None, None, None),
            P(AXES, None),
            P(AXES, None, None),
            P(AXES, None, None),
            P(AXES),
            P(AXES, None, None),
            P(),
        ),
        out_specs=P(AXES, None, None),
        check_vma=False,
    )
```

```python
import functools

import jax
import jax.numpy as jnp
from jax import lax
from jax.experimental import pallas as pl
from jax.experimental.pallas import tpu as pltpu
from jax.sharding import PartitionSpec as P

CA = 2
META = 32
AXES = ("grp", "dev")
VMEM = pltpu.VMEM
SMEM = pltpu.SMEM
F32 = jnp.float32
BF16 = jnp.bfloat16


SPACES = {"v": VMEM, "s": SMEM, "h": pltpu.HBM}


def call(kernel, args, spaces, outs, scratch=(), flops=1, limit=None):
    nbytes = sum(a.size * a.dtype.itemsize for a in args)
    in_specs = [pl.BlockSpec(memory_space=SPACES[c]) for c in spaces]
    return pl.pallas_call(
        kernel,
        out_shape=[jax.ShapeDtypeStruct(*o) for o in outs],
        in_specs=in_specs,
        out_specs=[pl.BlockSpec(memory_space=VMEM) for _ in outs],
        scratch_shapes=list(scratch),
        cost_estimate=pl.CostEstimate(flops=flops, bytes_accessed=nbytes, transcendentals=0),
        compiler_params=pltpu.CompilerParams(vmem_limit_bytes=limit),
    )(*[pltpu.with_memory_space_constraint(a, pltpu.HBM) if c == "h" else a for a, c in zip(args, spaces)])


def rows(index, size):
    return pl.ds(pl.multiple_of(index * size, size), size)


def dot(a, b):
    return jnp.dot(a, b, preferred_element_type=F32)


def pack_kernel(r, b, s, agg_hbm, ghost_hbm, tent_hbm, out, agg, ghost, sems):
    copies = [
        pltpu.make_async_copy(agg_hbm, agg, sems.at[0]),
        pltpu.make_async_copy(ghost_hbm, ghost, sems.at[1]),
        pltpu.make_async_copy(tent_hbm, out.at[: r * b, :], sems.at[2]),
    ]
    for copy in copies:
        copy.start()
    copies[0].wait()
    copies[1].wait()
    sub = lax.broadcasted_iota(jnp.int32, (META, b), 0)
    meta = jnp.zeros((META, b), F32)
    for j in range(r):
        meta = jnp.where(sub == j, agg[j].astype(F32), meta)
    for side in range(2):
        for j in range(s):
            meta = jnp.where(sub == 16 + 8 * side + j, ghost[0, side, j].astype(F32), meta)
    out[r * b :, :] = meta.astype(BF16)
    copies[2].wait()


def smooth(r, b, dense, cols, placed, inv, damp, target, base=None):
    step = 4
    for t in range(r // step):
        half = dot(dense[t * step * b : (t + 1) * step * b, cols], placed).astype(BF16)
        for q in range(step):
            at = slice((t * step + q) * b, (t * step + q + 1) * b)
            value = -damp[0] * dot(inv[at, :], half[q * b : (q + 1) * b, :])
            if base is not None:
                value = base[at, :].astype(F32) + value
            target[at, :] = value.astype(BF16)


def place_ghosts(r, b, s, ghost, mine, pay, meta, placed):
    meta[...] = pay[r * b :, :].astype(F32)
    for j in range(s):
        row = jnp.clip(ghost[0, mine, j], 0, r - 1)
        block = pay[rows(row, b), :]
        here = jnp.broadcast_to(meta[pl.ds(row, 1), :], (b, b))
        for c in range(CA):
            placed[j * b : (j + 1) * b, c * b : (c + 1) * b] = jnp.where(here == c, block.astype(F32), 0.0).astype(BF16)


def wanted_rows(r, s, theirs, meta):
    found = []
    for j in range(s):
        value = jnp.max(meta[pl.ds(16 + 8 * theirs + j, 1), :])
        found.append(jnp.clip(value.astype(jnp.int32), 0, r - 1))
    return found


def own_kernel(
    r, k, b, s, cols_hbm, agg_hbm, par, damp, vals_hbm, inv_hbm, pay, dense, inv, p_own, cols, agg, vals, placed, sems
):
    def fetch(j):
        return pltpu.make_async_copy(vals_hbm.at[j], vals.at[j], sems.at[j])

    others = [
        pltpu.make_async_copy(cols_hbm, cols, sems.at[r]),
        pltpu.make_async_copy(agg_hbm, agg, sems.at[r + 1]),
        pltpu.make_async_copy(inv_hbm, inv, sems.at[r + 2]),
    ]
    others[0].start()
    others[1].start()
    for j in range(r):
        fetch(j).start()
    others[2].start()

    def clear(j, carry):
        dense[rows(j, b), :] = jnp.zeros((b, (r + 2 * s) * b), BF16)
        return carry

    lax.fori_loop(0, r, clear, 0)
    others[0].wait()
    others[1].wait()
    zero = jnp.zeros((b, b), BF16)
    for j in range(r):
        own = slice(j * b, (j + 1) * b)
        block = pay[own, :]
        here = agg[j]
        for c in range(CA):
            placed[own, c * b : (c + 1) * b] = jnp.where(here == c, block, zero)
    odd = par[0]
    left = s * (1 - odd)

    def row(j, carry):
        fetch(j).wait()
        at = rows(j, b)
        for e in range(k):
            c = cols[j, e]
            c = jnp.where(c < r, c, jnp.where(c < r + s, c + left, c - left))
            dense[at, rows(c, b)] = vals[j, e]
        return carry

    lax.fori_loop(0, r, row, 0)
    others[2].wait()
    smooth(r, b, dense, slice(0, r * b), placed[...], inv, damp, p_own, placed)


def near_kernel(r, b, s, ghost, par, damp, dense, inv, p_own, pay, p_s, applied, meta, placed):
    place_ghosts(r, b, s, ghost, 1 - par[0], pay, meta, placed)
    smooth(r, b, dense, slice(r * b, (r + s) * b), placed[...], inv, damp, p_s)
    w = CA * b
    step = 4
    for t in range(r // step):
        at = slice(t * step * b, (t + 1) * step * b)
        block = dense[at, : r * b]
        applied[at, :w] = dot(block, p_s[...]).astype(BF16)
        applied[at, w:] = dot(block, p_own[...]).astype(BF16)


def far_kernel(r, b, s, ghost, par, damp, dense, inv, p_s, p_own, pay_s, pay_x, p_x, out_x, out_s, meta, near, placed):
    odd = par[0]
    place_ghosts(r, b, s, ghost, odd, pay_x, meta, placed)
    near[...] = pay_s[r * b :, :].astype(F32)
    wanted = (wanted_rows(r, s, 1 - odd, meta), wanted_rows(r, s, odd, near))
    smooth(r, b, dense, slice((r + s) * b, (r + 2 * s) * b), placed[...], inv, damp, p_x)
    w = CA * b
    for found, out in zip(wanted, (out_x, out_s)):
        for j in range(s):
            at = rows(found[j], b)
            to = slice(j * b, (j + 1) * b)
            out[to, :w] = p_s[at, :]
            out[to, w : 2 * w] = p_own[at, :]
            out[to, 2 * w :] = p_x[at, :]


def flip(r, b, p, flipped, d, w):
    for j in range(r):
        at = slice(j * b, (j + 1) * b)
        flipped[d * w : (d + 1) * w, at] = p[at, :].T


def cross_kernel(r, b, w, dense, p_x, applied, gal, wide, applied_x, flipped):
    flip(r, b, p_x, flipped, 0, w)
    step = 4
    for t in range(r // step):
        at = slice(t * step * b, (t + 1) * step * b)
        applied_x[at, :] = dot(dense[at, : r * b], p_x[...]).astype(BF16)
    left = flipped[...]
    wide[...] = dot(left, dense[:, r * b :]).astype(BF16)
    gal[:, : 2 * w] = dot(left, applied[...])
    gal[:, 2 * w :] = dot(left, applied_x[...])


def outer_kernel(w, span, gal, wide, far_s, out):
    by_s = dot(wide[:, :span], far_s[...])
    out[:, :w] = by_s[:, 2 * w :].astype(BF16)
    out[:, w : 2 * w] = (gal[:, :w] + by_s[:, w : 2 * w]).astype(BF16)
    out[:, 2 * w : 3 * w] = (gal[:, w : 2 * w] + by_s[:, :w]).astype(BF16)
    out[:, 3 * w : 4 * w] = gal[:, 2 * w :].astype(BF16)
    out[:, 4 * w :] = wide[:, span:]


def rest_kernel(r, b, w, dense, p_s, p_own, applied, applied_x, gal, wide, flipped):
    for d, p in enumerate((p_s, p_own)):
        flip(r, b, p, flipped, d, w)
    for d in range(2):
        at = slice(d * w, (d + 1) * w)
        left = flipped[at, :]
        wide[at, :] = dot(left, dense[:, r * b :]).astype(BF16)
        gal[at, : 2 * w] = dot(left, applied[...])
        gal[at, 2 * w :] = dot(left, applied_x[...])


def galerkin_rows(index, w, span, gal, wide, far_s, far_x):
    at = slice(index * w, (index + 1) * w)
    by_s = dot(wide[at, :span], far_s[...])
    by_x = dot(wide[at, span:], far_x[...])
    return (
        by_s[:, 2 * w :],
        gal[at, :w] + by_s[:, w : 2 * w],
        gal[at, w : 2 * w] + by_s[:, :w] + by_x[:, 2 * w :],
        gal[at, 2 * w :] + by_x[:, w : 2 * w],
        by_x[:, :w],
    )


def chip_kernel(w, span, gal, wide, far_s, far_x, out):
    for c, value in enumerate(galerkin_rows(0, w, span, gal, wide, far_s, far_x)):
        out[:, c * w : (c + 1) * w] = value.astype(BF16)


def inner_kernel(w, span, gal, wide, far_s, far_x, from_s, out):
    mine = galerkin_rows(1, w, span, gal, wide, far_s, far_x)
    for u in range(-3, 4):
        total = mine[2 - u] if abs(u) < 3 else jnp.zeros((w, w), F32)
        if 0 <= 1 + u < 5:
            total = total + from_s[:, (1 + u) * w : (2 + u) * w].astype(F32)
        out[:, (3 - u) * w : (4 - u) * w] = total


def final_kernel(w, par, mine, sent_x, from_x, out):
    sign = 1 - 2 * par[0]
    back = dot(from_x[:, 4 * w :], sent_x[...])
    for u in range(-3, 4):
        total = mine[:, (3 - u) * w : (4 - u) * w]
        if 0 <= 3 + u < 4:
            total = total + from_x[:, (3 + u) * w : (4 + u) * w].astype(F32)
        if abs(u) < 2:
            total = total + back[:, (1 - u) * w : (2 - u) * w]
        out[:, rows(3 + sign * u, w)] = total.astype(BF16)


def swap(x, route):
    return lax.ppermute(x, AXES, route)


def shards(block_values, block_columns, tentative, inverse_diagonal, aggregate, ghost_rows, damping):
    r, k = block_columns.shape
    b = tentative.shape[1]
    s = ghost_rows.shape[2]
    w = CA * b
    span = s * b
    devices = lax.axis_size(AXES)
    chip = [(i, i ^ 1) for i in range(devices) if i ^ 1 < devices]
    cross = []
    for i in range(1, devices - 1, 2):
        cross += [(i, i + 1), (i + 1, i)]
    par = (lax.axis_index(AXES) % 2).astype(jnp.int32).reshape(1)
    tent = tentative.reshape(r * b, b)
    inv = inverse_diagonal.reshape(r * b, b)
    dma = pltpu.SemaphoreType.DMA

    (pay,) = call(
        functools.partial(pack_kernel, r, b, s), (aggregate, ghost_rows, tent), "hhh",
        [((r * b + META, b), BF16)],
        scratch=[SMEM((r,), jnp.int32), SMEM((1, 2, s), jnp.int32), dma((3,))], limit=2 << 20,
    )
    pay_x = swap(pay, cross)
    pay_s = swap(pay, chip)
    dense, inv, p_own = call(
        functools.partial(own_kernel, r, k, b, s),
        (block_columns, aggregate, par, damping, block_values, inv, pay), "hhsshhv",
        [((r * b, (r + 2 * s) * b), BF16), ((r * b, b), BF16), ((r * b, w), BF16)],
        scratch=[
            SMEM((r, k), jnp.int32), SMEM((r,), jnp.int32), VMEM((r, k, b, b), BF16), VMEM((r * b, w), BF16),
            dma((r + 3,)),
        ],
        flops=2 * r * b * r * b * w, limit=24 << 20,
    )
    p_s, applied = call(
        functools.partial(near_kernel, r, b, s), (ghost_rows, par, damping, dense, inv, p_own, pay_s), "sssvvvv",
        [((r * b, w), BF16), ((r * b, 2 * w), BF16)],
        scratch=[VMEM((META, b), F32), VMEM((span, w), BF16)],
        flops=4 * r * b * r * b * w, limit=24 << 20,
    )
    p_x, out_x, out_s = call(
        functools.partial(far_kernel, r, b, s),
        (ghost_rows, par, damping, dense, inv, p_s, p_own, pay_s, pay_x), "sssvvvvvv",
        [((r * b, w), BF16), ((span, 3 * w), BF16), ((span, 3 * w), BF16)],
        scratch=[VMEM((META, b), F32), VMEM((META, b), F32), VMEM((span, w), BF16)],
        flops=2 * r * b * span * w, limit=24 << 20,
    )
    far_x = swap(out_x, cross)
    far_s = swap(out_s, chip)
    gal_x, wide_x, applied_x = call(
        functools.partial(cross_kernel, r, b, w), (dense, p_x, applied), "vvv",
        [((w, 3 * w), F32), ((w, 2 * span), BF16), ((r * b, w), BF16)],
        scratch=[VMEM((w, r * b), BF16)],
        flops=2 * r * b * r * b * 2 * w, limit=24 << 20,
    )
    (sum_x,) = call(
        functools.partial(outer_kernel, w, span), (gal_x, wide_x, far_s), "vvv",
        [((w, 4 * w + span), BF16)], flops=2 * w * span * 3 * w, limit=16 << 20,
    )
    from_x = swap(sum_x, cross)
    gal, wide = call(
        functools.partial(rest_kernel, r, b, w), (dense, p_s, p_own, applied, applied_x), "vvvvv",
        [((2 * w, 3 * w), F32), ((2 * w, 2 * span), BF16)],
        scratch=[VMEM((2 * w, r * b), BF16)],
        flops=2 * r * b * r * b * 2 * w, limit=24 << 20,
    )
    (sum_s,) = call(
        functools.partial(chip_kernel, w, span), (gal, wide, far_s, far_x), "vvvv",
        [((w, 5 * w), BF16)], flops=4 * w * span * 3 * w, limit=16 << 20,
    )
    from_s = swap(sum_s, chip)
    (mine,) = call(
        functools.partial(inner_kernel, w, span), (gal, wide, far_s, far_x, from_s), "vvvvv",
        [((w, 7 * w), F32)], flops=4 * w * span * 3 * w, limit=16 << 20,
    )
    (out,) = call(
        functools.partial(final_kernel, w), (par, mine, out_x, from_x), "svvv",
        [((w, 7 * w), BF16)], flops=2 * w * span * 3 * w, limit=16 << 20,
    )
    return out.reshape(CA, b, 7 * w)


def solution(mesh):
    return jax.shard_map(
        shards,
        mesh=mesh,
        in_specs=(
            P(AXES, None, None, None),
            P(AXES, None),
            P(AXES, None, None),
            P(AXES, None, None),
            P(AXES),
            P(AXES, None, None),
            P(),
        ),
        out_specs=P(AXES, None, None),
        check_vma=False,
    )
```

```python
import functools

import jax
import jax.numpy as jnp
from jax import lax
from jax.experimental import pallas as pl
from jax.experimental.pallas import tpu as pltpu
from jax.sharding import PartitionSpec as P

CA = 2
META = 32
AXES = ("grp", "dev")
VMEM = pltpu.VMEM
SMEM = pltpu.SMEM
F32 = jnp.float32
BF16 = jnp.bfloat16


SPACES = {"v": VMEM, "s": SMEM, "h": pltpu.HBM}


def call(kernel, args, spaces, outs, scratch=(), flops=1, limit=None, aliases=None, out_space=VMEM):
    nbytes = sum(a.size * a.dtype.itemsize for a in args)
    in_specs = [pl.BlockSpec(memory_space=SPACES[c]) for c in spaces]
    return pl.pallas_call(
        kernel,
        out_shape=[jax.ShapeDtypeStruct(*o) for o in outs],
        in_specs=in_specs,
        out_specs=[pl.BlockSpec(memory_space=out_space) for _ in outs],
        scratch_shapes=list(scratch),
        input_output_aliases=aliases or {},
        cost_estimate=pl.CostEstimate(flops=flops, bytes_accessed=nbytes, transcendentals=0),
        compiler_params=pltpu.CompilerParams(vmem_limit_bytes=limit),
    )(*[pltpu.with_memory_space_constraint(a, pltpu.HBM) if c == "h" else a for a, c in zip(args, spaces)])


def rows(index, size):
    return pl.ds(pl.multiple_of(index * size, size), size)


def dot(a, b):
    return jnp.dot(a, b, preferred_element_type=F32)


def pack_kernel(
    r, k, b, s, par, early, damp, agg_hbm, ghost_hbm, tent_hbm, cols_hbm, vals_hbm, inv_hbm,
    out, dense, inv, p_own, agg, ghost, cols, vals, placed, sems, own_sems,
):
    copies = [
        pltpu.make_async_copy(agg_hbm, agg, sems.at[0]),
        pltpu.make_async_copy(ghost_hbm, ghost, sems.at[1]),
        pltpu.make_async_copy(tent_hbm, out.at[: r * b, :], sems.at[2]),
    ]
    for copy in copies:
        copy.start()
    copies[0].wait()
    copies[1].wait()
    sub = lax.broadcasted_iota(jnp.int32, (META, b), 0)
    meta = jnp.zeros((META, b), F32)
    for j in range(r):
        meta = jnp.where(sub == j, agg[j].astype(F32), meta)
    for side in range(2):
        for j in range(s):
            meta = jnp.where(sub == 16 + 8 * side + j, ghost[0, side, j].astype(F32), meta)
    out[r * b :, :] = meta.astype(BF16)
    copies[2].wait()

    @pl.when(early[0] == 1)
    def _():
        own_rows(
            r, k, b, s, par, damp, agg_hbm, cols_hbm, vals_hbm, inv_hbm, out, dense, inv, p_own, agg, cols, vals,
            placed, own_sems,
        )


def own_kernel(
    r, k, b, s, par, early, damp, agg_hbm, cols_hbm, vals_hbm, inv_hbm, pay, dense_in, inv_in, p_own_in,
    dense, inv, p_own, agg, cols, vals, placed, sems,
):
    @pl.when(early[0] == 0)
    def _():
        own_rows(
            r, k, b, s, par, damp, agg_hbm, cols_hbm, vals_hbm, inv_hbm, pay, dense, inv, p_own, agg, cols, vals,
            placed, sems,
        )


def smooth(r, b, dense, cols, placed, inv, damp, target, base=None):
    step = 4
    for t in range(r // step):
        half = dot(dense[t * step * b : (t + 1) * step * b, cols], placed).astype(BF16)
        for q in range(step):
            at = slice((t * step + q) * b, (t * step + q + 1) * b)
            value = -damp[0] * dot(inv[at, :], half[q * b : (q + 1) * b, :])
            if base is not None:
                value = base[at, :].astype(F32) + value
            target[at, :] = value.astype(BF16)


def place_ghosts(r, b, s, ghost, mine, pay, meta, placed):
    meta[...] = pay[r * b :, :].astype(F32)
    for j in range(s):
        row = jnp.clip(ghost[0, mine, j], 0, r - 1)
        block = pay[rows(row, b), :]
        here = jnp.broadcast_to(meta[pl.ds(row, 1), :], (b, b))
        for c in range(CA):
            placed[j * b : (j + 1) * b, c * b : (c + 1) * b] = jnp.where(here == c, block.astype(F32), 0.0).astype(BF16)


def wanted_rows(r, s, theirs, meta):
    found = []
    for j in range(s):
        value = jnp.max(meta[pl.ds(16 + 8 * theirs + j, 1), :])
        found.append(jnp.clip(value.astype(jnp.int32), 0, r - 1))
    return found


def own_rows(
    r, k, b, s, par, damp, agg_hbm, cols_hbm, vals_hbm, inv_hbm, pay, dense, inv, p_own, agg, cols, vals, placed, sems
):
    def fetch(j):
        return pltpu.make_async_copy(vals_hbm.at[j], vals.at[j], sems.at[j])

    others = [
        pltpu.make_async_copy(cols_hbm, cols, sems.at[r]),
        pltpu.make_async_copy(agg_hbm, agg, sems.at[r + 1]),
        pltpu.make_async_copy(inv_hbm, inv, sems.at[r + 2]),
    ]
    others[0].start()
    others[1].start()
    for j in range(r):
        fetch(j).start()
    others[2].start()

    def clear(j, carry):
        dense[rows(j, b), :] = jnp.zeros((b, (r + 2 * s) * b), BF16)
        return carry

    lax.fori_loop(0, r, clear, 0)
    others[0].wait()
    others[1].wait()
    zero = jnp.zeros((b, b), BF16)
    for j in range(r):
        own = slice(j * b, (j + 1) * b)
        block = pay[own, :]
        here = agg[j]
        for c in range(CA):
            placed[own, c * b : (c + 1) * b] = jnp.where(here == c, block, zero)
    odd = par[0]
    left = s * (1 - odd)

    def row(j, carry):
        fetch(j).wait()
        at = rows(j, b)
        for e in range(k):
            c = cols[j, e]
            c = jnp.where(c < r, c, jnp.where(c < r + s, c + left, c - left))
            dense[at, rows(c, b)] = vals[j, e]
        return carry

    lax.fori_loop(0, r, row, 0)
    others[2].wait()
    smooth(r, b, dense, slice(0, r * b), placed[...], inv, damp, p_own, placed)


def near_kernel(r, b, s, ghost, par, damp, dense, inv, p_own, pay, p_s, y_own, meta, placed, flipped):
    flip(r, b, p_own, flipped)
    place_ghosts(r, b, s, ghost, 1 - par[0], pay, meta, placed)
    smooth(r, b, dense, slice(r * b, (r + s) * b), placed[...], inv, damp, p_s)
    y_own[...] = dot(flipped[...], dense[...]).astype(BF16)


def far_kernel(
    r, b, s, w, ghost, par, early, damp, dense, inv, p_s, p_own, pay_s, pay_x,
    p_x, out_x, out_s, y_x, gal_x, meta, near, placed, flipped,
):
    odd = par[0]
    place_ghosts(r, b, s, ghost, odd, pay_x, meta, placed)
    near[...] = pay_s[r * b :, :].astype(F32)
    wanted = (wanted_rows(r, s, 1 - odd, meta), wanted_rows(r, s, odd, near))
    smooth(r, b, dense, slice((r + s) * b, (r + 2 * s) * b), placed[...], inv, damp, p_x)
    for found, out in zip(wanted, (out_x, out_s)):
        for j in range(s):
            at = rows(found[j], b)
            to = slice(j * b, (j + 1) * b)
            out[to, :w] = p_s[at, :]
            out[to, w : 2 * w] = p_own[at, :]
            out[to, 2 * w :] = p_x[at, :]

    @pl.when(early[0] == 1)
    def _():
        part_rows(r, b, w, dense, p_x, (p_s, p_own, p_x), y_x, gal_x, flipped)


def cross_kernel(r, b, w, early, dense, p_s, p_own, p_x, y_in, gal_in, y_x, gal_x, flipped):
    @pl.when(early[0] == 0)
    def _():
        part_rows(r, b, w, dense, p_x, (p_s, p_own, p_x), y_x, gal_x, flipped)


def flip(r, b, p, flipped):
    for j in range(r):
        at = slice(j * b, (j + 1) * b)
        flipped[:, at] = p[at, :].T


def part_rows(r, b, w, dense, p, parts, y, gal, flipped):
    flip(r, b, p, flipped)
    y[...] = dot(flipped[...], dense[...]).astype(BF16)
    for d, other in enumerate(parts):
        gal[:, d * w : (d + 1) * w] = dot(y[:, : r * b], other[...])


def outer_kernel(w, span, gal, y, far_s, out):
    own = y.shape[1] - 2 * span
    by_s = dot(y[:, own : own + span], far_s[...])
    out[:, :w] = by_s[:, 2 * w :].astype(BF16)
    out[:, w : 2 * w] = (gal[:, :w] + by_s[:, w : 2 * w]).astype(BF16)
    out[:, 2 * w : 3 * w] = (gal[:, w : 2 * w] + by_s[:, :w]).astype(BF16)
    out[:, 3 * w : 4 * w] = gal[:, 2 * w :].astype(BF16)
    out[:, 4 * w :] = y[:, own + span :]


def rest_kernel(r, b, w, dense, p_s, p_own, p_x, y_own, y_s, gal_s, gal_own, flipped):
    parts = (p_s, p_own, p_x)
    for d, other in enumerate(parts):
        gal_own[:, d * w : (d + 1) * w] = dot(y_own[:, : r * b], other[...])
    part_rows(r, b, w, dense, p_s, parts, y_s, gal_s, flipped)


def galerkin_rows(w, span, gal, y, far_s, far_x):
    own = y.shape[1] - 2 * span
    by_s = dot(y[:, own : own + span], far_s[...])
    by_x = dot(y[:, own + span :], far_x[...])
    return (
        by_s[:, 2 * w :],
        gal[:, :w] + by_s[:, w : 2 * w],
        gal[:, w : 2 * w] + by_s[:, :w] + by_x[:, 2 * w :],
        gal[:, 2 * w :] + by_x[:, w : 2 * w],
        by_x[:, :w],
    )


def chip_kernel(w, span, gal, y, far_s, far_x, out):
    for c, value in enumerate(galerkin_rows(w, span, gal, y, far_s, far_x)):
        out[:, c * w : (c + 1) * w] = value.astype(BF16)


def inner_kernel(w, span, gal, y, far_s, far_x, from_s, out):
    mine = galerkin_rows(w, span, gal, y, far_s, far_x)
    for u in range(-3, 4):
        total = mine[2 - u] if abs(u) < 3 else jnp.zeros((w, w), F32)
        if 0 <= 1 + u < 5:
            total = total + from_s[:, (1 + u) * w : (2 + u) * w].astype(F32)
        out[:, (3 - u) * w : (4 - u) * w] = total


def final_kernel(w, par, mine, sent_x, from_x, out_hbm, out, sems):
    sign = 1 - 2 * par[0]
    back = dot(from_x[:, 4 * w :], sent_x[...])
    copies = []
    for u in (3, 2, -3, -2, -1, 0, 1):
        total = mine[:, (3 - u) * w : (4 - u) * w]
        if 0 <= 3 + u < 4:
            total = total + from_x[:, (3 + u) * w : (4 + u) * w].astype(F32)
        if abs(u) < 2:
            total = total + back[:, (1 - u) * w : (2 - u) * w]
        out[u + 3, :, :] = total.astype(BF16)
        copies.append(pltpu.make_async_copy(out.at[u + 3], out_hbm.at[:, rows(3 + sign * u, w)], sems.at[u + 3]))
        copies[-1].start()
    for copy in copies:
        copy.wait()


def swap(x, route):
    return lax.ppermute(x, AXES, route)


def shards(block_values, block_columns, tentative, inverse_diagonal, aggregate, ghost_rows, damping):
    r, k = block_columns.shape
    b = tentative.shape[1]
    s = ghost_rows.shape[2]
    w = CA * b
    span = s * b
    devices = lax.axis_size(AXES)
    chip = [(i, i ^ 1) for i in range(devices) if i ^ 1 < devices]
    cross = []
    for i in range(1, devices - 1, 2):
        cross += [(i, i + 1), (i + 1, i)]
    grp, dev = (lax.axis_index(a) for a in AXES)
    par = (dev & 1).astype(jnp.int32).reshape(1)
    early = ((dev == 0) & (grp > 0)).astype(jnp.int32).reshape(1)
    tent = tentative.reshape(r * b, b)
    inv_hbm = inverse_diagonal.reshape(r * b, b)
    dma = pltpu.SemaphoreType.DMA
    total = (r + 2 * s) * b
    own_outs = [((r * b, total), BF16), ((r * b, b), BF16), ((r * b, w), BF16)]
    own_scratch = [SMEM((r, k), jnp.int32), VMEM((r, k, b, b), BF16), VMEM((r * b, w), BF16)]

    pay, dense, inv, p_own = call(
        functools.partial(pack_kernel, r, k, b, s),
        (par, early, damping, aggregate, ghost_rows, tent, block_columns, block_values, inv_hbm), "ssshhhhhh",
        [((r * b + META, b), BF16)] + own_outs,
        scratch=[SMEM((r,), jnp.int32), SMEM((1, 2, s), jnp.int32)] + own_scratch + [dma((3,)), dma((r + 3,))],
        limit=24 << 20,
    )
    pay_x = swap(pay, cross)
    pay_s = swap(pay, chip)
    dense, inv, p_own = call(
        functools.partial(own_kernel, r, k, b, s),
        (par, early, damping, aggregate, block_columns, block_values, inv_hbm, pay, dense, inv, p_own), "ssshhhhvvvv",
        own_outs, scratch=[SMEM((r,), jnp.int32)] + own_scratch + [dma((r + 3,))],
        flops=2 * r * b * r * b * w, limit=24 << 20, aliases={8: 0, 9: 1, 10: 2},
    )
    p_s, y_own = call(
        functools.partial(near_kernel, r, b, s), (ghost_rows, par, damping, dense, inv, p_own, pay_s), "sssvvvv",
        [((r * b, w), BF16), ((w, total), BF16)],
        scratch=[VMEM((META, b), F32), VMEM((span, w), BF16), VMEM((w, r * b), BF16)],
        flops=2 * r * b * total * w, limit=24 << 20,
    )
    p_x, out_x, out_s, y_x, gal_x = call(
        functools.partial(far_kernel, r, b, s, w),
        (ghost_rows, par, early, damping, dense, inv, p_s, p_own, pay_s, pay_x), "ssssvvvvvv",
        [((r * b, w), BF16), ((span, 3 * w), BF16), ((span, 3 * w), BF16), ((w, total), BF16), ((w, 3 * w), F32)],
        scratch=[VMEM((META, b), F32), VMEM((META, b), F32), VMEM((span, w), BF16), VMEM((w, r * b), BF16)],
        flops=2 * r * b * span * w, limit=24 << 20,
    )
    far_x = swap(out_x, cross)
    far_s = swap(out_s, chip)
    y_x, gal_x = call(
        functools.partial(cross_kernel, r, b, w), (early, dense, p_s, p_own, p_x, y_x, gal_x), "svvvvvv",
        [((w, total), BF16), ((w, 3 * w), F32)], scratch=[VMEM((w, r * b), BF16)],
        flops=2 * r * b * r * b * 2 * w, limit=24 << 20, aliases={5: 0, 6: 1},
    )
    (sum_x,) = call(
        functools.partial(outer_kernel, w, span), (gal_x, y_x, far_s), "vvv",
        [((w, 4 * w + span), BF16)], flops=2 * w * span * 3 * w, limit=16 << 20,
    )
    from_x = swap(sum_x, cross)
    y_s, gal_s, gal_own = call(
        functools.partial(rest_kernel, r, b, w), (dense, p_s, p_own, p_x, y_own), "vvvvv",
        [((w, total), BF16), ((w, 3 * w), F32), ((w, 3 * w), F32)], scratch=[VMEM((w, r * b), BF16)],
        flops=2 * r * b * r * b * 2 * w, limit=24 << 20,
    )
    (sum_s,) = call(
        functools.partial(chip_kernel, w, span), (gal_s, y_s, far_s, far_x), "vvvv",
        [((w, 5 * w), BF16)], flops=4 * w * span * 3 * w, limit=16 << 20,
    )
    from_s = swap(sum_s, chip)
    (mine,) = call(
        functools.partial(inner_kernel, w, span), (gal_own, y_own, far_s, far_x, from_s), "vvvvv",
        [((w, 7 * w), F32)], flops=4 * w * span * 3 * w, limit=16 << 20,
    )
    (out,) = call(
        functools.partial(final_kernel, w), (par, mine, out_x, from_x), "svvv",
        [((w, 7 * w), BF16)], scratch=[VMEM((7, w, w), BF16), dma((7,))],
        flops=2 * w * span * 3 * w, limit=16 << 20, out_space=pltpu.HBM,
    )
    return out.reshape(CA, b, 7 * w)


def solution(mesh):
    return jax.shard_map(
        shards,
        mesh=mesh,
        in_specs=(
            P(AXES, None, None, None),
            P(AXES, None),
            P(AXES, None, None),
            P(AXES, None, None),
            P(AXES),
            P(AXES, None, None),
            P(),
        ),
        out_specs=P(AXES, None, None),
        check_vma=False,
    )
```

```python
import functools

import jax
import jax.numpy as jnp
from jax import lax
from jax.experimental import pallas as pl
from jax.experimental.pallas import tpu as pltpu
from jax.sharding import PartitionSpec as P

CA = 2
META = 32
AXES = ("grp", "dev")
VMEM = pltpu.VMEM
SMEM = pltpu.SMEM
F32 = jnp.float32
BF16 = jnp.bfloat16


SPACES = {"v": VMEM, "s": SMEM, "h": pltpu.HBM}


def call(kernel, args, spaces, outs, scratch=(), flops=1, limit=None, aliases=None, out_space=VMEM):
    nbytes = sum(a.size * a.dtype.itemsize for a in args)
    in_specs = [pl.BlockSpec(memory_space=SPACES[c]) for c in spaces]
    return pl.pallas_call(
        kernel,
        out_shape=[jax.ShapeDtypeStruct(*o) for o in outs],
        in_specs=in_specs,
        out_specs=[pl.BlockSpec(memory_space=out_space) for _ in outs],
        scratch_shapes=list(scratch),
        input_output_aliases=aliases or {},
        cost_estimate=pl.CostEstimate(flops=flops, bytes_accessed=nbytes, transcendentals=0),
        compiler_params=pltpu.CompilerParams(vmem_limit_bytes=limit),
    )(*[pltpu.with_memory_space_constraint(a, pltpu.HBM) if c == "h" else a for a, c in zip(args, spaces)])


def rows(index, size):
    return pl.ds(pl.multiple_of(index * size, size), size)


def dot(a, b):
    return jnp.dot(a, b, preferred_element_type=F32)


def pack_kernel(r, b, s, agg_hbm, ghost_hbm, tent_hbm, out, agg, ghost, sems):
    copies = [
        pltpu.make_async_copy(agg_hbm, agg, sems.at[0]),
        pltpu.make_async_copy(ghost_hbm, ghost, sems.at[1]),
        pltpu.make_async_copy(tent_hbm, out.at[: r * b, :], sems.at[2]),
    ]
    for copy in copies:
        copy.start()
    copies[0].wait()
    copies[1].wait()
    sub = lax.broadcasted_iota(jnp.int32, (META, b), 0)
    meta = jnp.zeros((META, b), F32)
    for j in range(r):
        meta = jnp.where(sub == j, agg[j].astype(F32), meta)
    for side in range(2):
        for j in range(s):
            meta = jnp.where(sub == 16 + 8 * side + j, ghost[0, side, j].astype(F32), meta)
    out[r * b :, :] = meta.astype(BF16)
    copies[2].wait()


def smooth(r, b, dense, cols, placed, inv, damp, target, base=None):
    step = 4
    for t in range(r // step):
        half = dot(dense[t * step * b : (t + 1) * step * b, cols], placed).astype(BF16)
        for q in range(step):
            at = slice((t * step + q) * b, (t * step + q + 1) * b)
            value = -damp[0] * dot(inv[at, :], half[q * b : (q + 1) * b, :])
            if base is not None:
                value = base[at, :].astype(F32) + value
            target[at, :] = value.astype(BF16)


def place_ghosts(r, b, s, ghost, mine, pay, meta, placed):
    meta[...] = pay[r * b :, :].astype(F32)
    for j in range(s):
        row = jnp.clip(ghost[0, mine, j], 0, r - 1)
        block = pay[rows(row, b), :]
        here = jnp.broadcast_to(meta[pl.ds(row, 1), :], (b, b))
        for c in range(CA):
            placed[j * b : (j + 1) * b, c * b : (c + 1) * b] = jnp.where(here == c, block.astype(F32), 0.0).astype(BF16)


def wanted_rows(r, s, theirs, meta):
    found = []
    for j in range(s):
        value = jnp.max(meta[pl.ds(16 + 8 * theirs + j, 1), :])
        found.append(jnp.clip(value.astype(jnp.int32), 0, r - 1))
    return found


def own_kernel(
    r, k, b, s, par, damp, agg_hbm, cols_hbm, vals_hbm, inv_hbm, pay, dense, inv, p_own, agg, cols, vals, placed, sems
):
    def fetch(j):
        return pltpu.make_async_copy(vals_hbm.at[j], vals.at[j], sems.at[j])

    others = [
        pltpu.make_async_copy(cols_hbm, cols, sems.at[r]),
        pltpu.make_async_copy(agg_hbm, agg, sems.at[r + 1]),
        pltpu.make_async_copy(inv_hbm, inv, sems.at[r + 2]),
    ]
    others[0].start()
    others[1].start()
    for j in range(r):
        fetch(j).start()
    others[2].start()

    def clear(j, carry):
        dense[rows(j, b), :] = jnp.zeros((b, (r + 2 * s) * b), BF16)
        return carry

    lax.fori_loop(0, r, clear, 0)
    others[0].wait()
    others[1].wait()
    zero = jnp.zeros((b, b), BF16)
    for j in range(r):
        own = slice(j * b, (j + 1) * b)
        block = pay[own, :]
        here = agg[j]
        for c in range(CA):
            placed[own, c * b : (c + 1) * b] = jnp.where(here == c, block, zero)
    odd = par[0]
    left = s * (1 - odd)

    def row(j, carry):
        fetch(j).wait()
        at = rows(j, b)
        for e in range(k):
            c = cols[j, e]
            c = jnp.where(c < r, c, jnp.where(c < r + s, c + left, c - left))
            dense[at, rows(c, b)] = vals[j, e]
        return carry

    lax.fori_loop(0, r, row, 0)
    others[2].wait()
    smooth(r, b, dense, slice(0, r * b), placed[...], inv, damp, p_own, placed)


def near_kernel(r, b, s, ghost, par, damp, dense, inv, pay, p_s, meta, placed):
    place_ghosts(r, b, s, ghost, 1 - par[0], pay, meta, placed)
    smooth(r, b, dense, slice(r * b, (r + s) * b), placed[...], inv, damp, p_s)


def far_kernel(r, b, s, w, ghost, par, damp, dense, inv, p_s, p_own, pay_s, pay_x, p_x, out_x, out_s, meta, near, placed):
    odd = par[0]
    place_ghosts(r, b, s, ghost, odd, pay_x, meta, placed)
    near[...] = pay_s[r * b :, :].astype(F32)
    wanted = (wanted_rows(r, s, 1 - odd, meta), wanted_rows(r, s, odd, near))
    smooth(r, b, dense, slice((r + s) * b, (r + 2 * s) * b), placed[...], inv, damp, p_x)
    for found, out in zip(wanted, (out_x, out_s)):
        for j in range(s):
            at = rows(found[j], b)
            to = slice(j * b, (j + 1) * b)
            out[to, :w] = p_s[at, :]
            out[to, w : 2 * w] = p_own[at, :]
            out[to, 2 * w :] = p_x[at, :]


def cross_kernel(parity, r, b, w, par, dense, p_s, p_own, p_x, far_s, *refs):
    out, y_own, y, flipped = refs[-4:]

    @pl.when(par[0] == parity)
    def _():
        flip(r, b, p_x, flipped)
        y[...] = dot(flipped[...], dense[...]).astype(BF16)
        inside = y[:, : r * b]
        own = r * b
        span = far_s.shape[0]
        by_s = dot(y[:, own : own + span], far_s[...])
        out[:, :w] = by_s[:, 2 * w :].astype(BF16)
        out[:, w : 2 * w] = (dot(inside, p_s[...]) + by_s[:, w : 2 * w]).astype(BF16)
        out[:, 2 * w : 3 * w] = (dot(inside, p_own[...]) + by_s[:, :w]).astype(BF16)
        out[:, 3 * w : 4 * w] = dot(inside, p_x[...]).astype(BF16)
        out[:, 4 * w :] = y[:, own + span :]
        flip(r, b, p_own, flipped)
        y_own[...] = dot(flipped[...], dense[...]).astype(BF16)


def flip(r, b, p, flipped):
    for j in range(r):
        at = slice(j * b, (j + 1) * b)
        flipped[:, at] = p[at, :].T


def part_rows(r, b, w, dense, p, parts, y, gal, flipped):
    flip(r, b, p, flipped)
    y[...] = dot(flipped[...], dense[...]).astype(BF16)
    for d, other in enumerate(parts):
        gal[:, d * w : (d + 1) * w] = dot(y[:, : r * b], other[...])


def rest_kernel(r, b, w, dense, p_s, p_own, p_x, y_own, y_s, gal_s, gal_own, flipped):
    parts = (p_s, p_own, p_x)
    for d, other in enumerate(parts):
        gal_own[:, d * w : (d + 1) * w] = dot(y_own[:, : r * b], other[...])
    part_rows(r, b, w, dense, p_s, parts, y_s, gal_s, flipped)


def galerkin_rows(w, span, gal, y, far_s, far_x):
    own = y.shape[1] - 2 * span
    by_s = dot(y[:, own : own + span], far_s[...])
    by_x = dot(y[:, own + span :], far_x[...])
    return (
        by_s[:, 2 * w :],
        gal[:, :w] + by_s[:, w : 2 * w],
        gal[:, w : 2 * w] + by_s[:, :w] + by_x[:, 2 * w :],
        gal[:, 2 * w :] + by_x[:, w : 2 * w],
        by_x[:, :w],
    )


def chip_kernel(w, span, gal, y, far_s, far_x, out):
    for c, value in enumerate(galerkin_rows(w, span, gal, y, far_s, far_x)):
        out[:, c * w : (c + 1) * w] = value.astype(BF16)


def inner_kernel(w, span, gal, y, far_s, far_x, from_s, out):
    mine = galerkin_rows(w, span, gal, y, far_s, far_x)
    for u in range(-3, 4):
        total = mine[2 - u] if abs(u) < 3 else jnp.zeros((w, w), F32)
        if 0 <= 1 + u < 5:
            total = total + from_s[:, (1 + u) * w : (2 + u) * w].astype(F32)
        out[:, (3 - u) * w : (4 - u) * w] = total


def final_kernel(w, par, mine, sent_x, from_odd, from_even, out_hbm, out, sems):
    def finish(sign, from_x):
        back = dot(from_x[:, 4 * w :], sent_x[...])
        copies = []
        for u in (3, 2, -3, -2, -1, 0, 1):
            total = mine[:, (3 - u) * w : (4 - u) * w]
            if 0 <= 3 + u < 4:
                total = total + from_x[:, (3 + u) * w : (4 + u) * w].astype(F32)
            if abs(u) < 2:
                total = total + back[:, (1 - u) * w : (2 - u) * w]
            out[u + 3, :, :] = total.astype(BF16)
            place = out_hbm.at[:, (3 + sign * u) * w : (4 + sign * u) * w]
            copies.append(pltpu.make_async_copy(out.at[u + 3], place, sems.at[u + 3]))
            copies[-1].start()
        for copy in copies:
            copy.wait()

    @pl.when(par[0] == 0)
    def _():
        finish(1, from_odd)

    @pl.when(par[0] == 1)
    def _():
        finish(-1, from_even)


def swap(x, route):
    return lax.ppermute(x, AXES, route)


def shards(block_values, block_columns, tentative, inverse_diagonal, aggregate, ghost_rows, damping):
    r, k = block_columns.shape
    b = tentative.shape[1]
    s = ghost_rows.shape[2]
    w = CA * b
    span = s * b
    devices = lax.axis_size(AXES)
    chip = [(i, i ^ 1) for i in range(devices) if i ^ 1 < devices]
    up = [(i, i + 1) for i in range(1, devices - 1, 2)]
    down = [(j, i) for i, j in up]
    _, dev = (lax.axis_index(a) for a in AXES)
    par = (dev & 1).astype(jnp.int32).reshape(1)
    tent = tentative.reshape(r * b, b)
    inv = inverse_diagonal.reshape(r * b, b)
    dma = pltpu.SemaphoreType.DMA
    total = (r + 2 * s) * b

    (pay,) = call(
        functools.partial(pack_kernel, r, b, s), (aggregate, ghost_rows, tent), "hhh",
        [((r * b + META, b), BF16)],
        scratch=[SMEM((r,), jnp.int32), SMEM((1, 2, s), jnp.int32), dma((3,))], limit=2 << 20,
    )
    pay_x = swap(pay, up + down)
    pay_s = swap(pay, chip)
    dense, inv, p_own = call(
        functools.partial(own_kernel, r, k, b, s),
        (par, damping, aggregate, block_columns, block_values, inv, pay), "sshhhhv",
        [((r * b, total), BF16), ((r * b, b), BF16), ((r * b, w), BF16)],
        scratch=[
            SMEM((r,), jnp.int32), SMEM((r, k), jnp.int32), VMEM((r, k, b, b), BF16), VMEM((r * b, w), BF16),
            dma((r + 3,)),
        ],
        flops=2 * r * b * r * b * w, limit=24 << 20,
    )
    (p_s,) = call(
        functools.partial(near_kernel, r, b, s), (ghost_rows, par, damping, dense, inv, pay_s), "sssvvv",
        [((r * b, w), BF16)], scratch=[VMEM((META, b), F32), VMEM((span, w), BF16)],
        flops=2 * r * b * span * w, limit=24 << 20,
    )
    p_x, out_x, out_s = call(
        functools.partial(far_kernel, r, b, s, w),
        (ghost_rows, par, damping, dense, inv, p_s, p_own, pay_s, pay_x), "sssvvvvvv",
        [((r * b, w), BF16), ((span, 3 * w), BF16), ((span, 3 * w), BF16)],
        scratch=[VMEM((META, b), F32), VMEM((META, b), F32), VMEM((span, w), BF16)],
        flops=2 * r * b * span * w, limit=24 << 20,
    )
    far_x = swap(out_x, up + down)
    far_s = swap(out_s, chip)
    shapes = [((w, 4 * w + span), BF16), ((w, total), BF16)]
    scratch = [VMEM((w, total), BF16), VMEM((w, r * b), BF16)]
    flops = 2 * r * b * r * b * 4 * w
    ready = (par, dense, p_s, p_own, p_x, far_s)
    sum_odd, y_own = call(
        functools.partial(cross_kernel, 1, r, b, w), ready, "svvvvv",
        shapes, scratch=scratch, flops=flops, limit=24 << 20,
    )
    from_odd = swap(sum_odd, up)
    sum_even, y_own = call(
        functools.partial(cross_kernel, 0, r, b, w), ready + (y_own,), "svvvvvv",
        shapes, scratch=scratch, flops=flops, limit=24 << 20, aliases={6: 1},
    )
    from_even = swap(sum_even, down)
    y_s, gal_s, gal_own = call(
        functools.partial(rest_kernel, r, b, w), (dense, p_s, p_own, p_x, y_own), "vvvvv",
        [((w, total), BF16), ((w, 3 * w), F32), ((w, 3 * w), F32)], scratch=[VMEM((w, r * b), BF16)],
        flops=2 * r * b * r * b * 2 * w, limit=24 << 20,
    )
    (sum_s,) = call(
        functools.partial(chip_kernel, w, span), (gal_s, y_s, far_s, far_x), "vvvv",
        [((w, 5 * w), BF16)], flops=4 * w * span * 3 * w, limit=16 << 20,
    )
    from_s = swap(sum_s, chip)
    (mine,) = call(
        functools.partial(inner_kernel, w, span), (gal_own, y_own, far_s, far_x, from_s), "vvvvv",
        [((w, 7 * w), F32)], flops=4 * w * span * 3 * w, limit=16 << 20,
    )
    (out,) = call(
        functools.partial(final_kernel, w), (par, mine, out_x, from_odd, from_even), "svvvv",
        [((w, 7 * w), BF16)], scratch=[VMEM((7, w, w), BF16), dma((7,))],
        flops=2 * w * span * 3 * w, limit=16 << 20, out_space=pltpu.HBM,
    )
    return out.reshape(CA, b, 7 * w)


def solution(mesh):
    return jax.shard_map(
        shards,
        mesh=mesh,
        in_specs=(
            P(AXES, None, None, None),
            P(AXES, None),
            P(AXES, None, None),
            P(AXES, None, None),
            P(AXES),
            P(AXES, None, None),
            P(),
        ),
        out_specs=P(AXES, None, None),
        check_vma=False,
    )
```

```python
import functools

import jax
import jax.numpy as jnp
from jax import lax
from jax.experimental import pallas as pl
from jax.experimental.pallas import tpu as pltpu
from jax.sharding import PartitionSpec as P

CA = 2
META = 32
AXES = ("grp", "dev")
VMEM = pltpu.VMEM
SMEM = pltpu.SMEM
F32 = jnp.float32
BF16 = jnp.bfloat16


SPACES = {"v": VMEM, "s": SMEM, "h": pltpu.HBM}


def call(kernel, args, spaces, outs, scratch=(), flops=1, limit=None, aliases=None, out_space=VMEM):
    nbytes = sum(a.size * a.dtype.itemsize for a in args)
    in_specs = [pl.BlockSpec(memory_space=SPACES[c]) for c in spaces]
    return pl.pallas_call(
        kernel,
        out_shape=[jax.ShapeDtypeStruct(*o) for o in outs],
        in_specs=in_specs,
        out_specs=[pl.BlockSpec(memory_space=out_space) for _ in outs],
        scratch_shapes=list(scratch),
        input_output_aliases=aliases or {},
        cost_estimate=pl.CostEstimate(flops=flops, bytes_accessed=nbytes, transcendentals=0),
        compiler_params=pltpu.CompilerParams(vmem_limit_bytes=limit),
    )(*[pltpu.with_memory_space_constraint(a, pltpu.HBM) if c == "h" else a for a, c in zip(args, spaces)])


def rows(index, size):
    return pl.ds(pl.multiple_of(index * size, size), size)


def dot(a, b):
    return jnp.dot(a, b, preferred_element_type=F32)


def pack_kernel(r, b, s, agg_hbm, ghost_hbm, tent_hbm, out, agg, ghost, sems):
    copies = [
        pltpu.make_async_copy(agg_hbm, agg, sems.at[0]),
        pltpu.make_async_copy(ghost_hbm, ghost, sems.at[1]),
        pltpu.make_async_copy(tent_hbm, out.at[: r * b, :], sems.at[2]),
    ]
    for copy in copies:
        copy.start()
    copies[0].wait()
    copies[1].wait()
    sub = lax.broadcasted_iota(jnp.int32, (META, b), 0)
    meta = jnp.zeros((META, b), F32)
    for j in range(r):
        meta = jnp.where(sub == j, agg[j].astype(F32), meta)
    for side in range(2):
        for j in range(s):
            meta = jnp.where(sub == 16 + 8 * side + j, ghost[0, side, j].astype(F32), meta)
    out[r * b :, :] = meta.astype(BF16)
    copies[2].wait()


def smooth(r, b, dense, cols, placed, inv, damp, target, base=None):
    step = 4
    for t in range(r // step):
        half = dot(dense[t * step * b : (t + 1) * step * b, cols], placed).astype(BF16)
        for q in range(step):
            at = slice((t * step + q) * b, (t * step + q + 1) * b)
            value = -damp[0] * dot(inv[at, :], half[q * b : (q + 1) * b, :])
            if base is not None:
                value = base[at, :].astype(F32) + value
            target[at, :] = value.astype(BF16)


def place_ghosts(r, b, s, ghost, mine, pay, meta, placed):
    meta[...] = pay[r * b :, :].astype(F32)
    for j in range(s):
        row = jnp.clip(ghost[0, mine, j], 0, r - 1)
        block = pay[rows(row, b), :]
        here = jnp.broadcast_to(meta[pl.ds(row, 1), :], (b, b))
        for c in range(CA):
            placed[j * b : (j + 1) * b, c * b : (c + 1) * b] = jnp.where(here == c, block.astype(F32), 0.0).astype(BF16)


def wanted_rows(r, s, theirs, meta):
    found = []
    for j in range(s):
        value = jnp.max(meta[pl.ds(16 + 8 * theirs + j, 1), :])
        found.append(jnp.clip(value.astype(jnp.int32), 0, r - 1))
    return found


def own_kernel(
    r, k, b, s, par, damp, agg_hbm, cols_hbm, vals_hbm, inv_hbm, pay, dense, inv, p_own, agg, cols, vals, placed, sems
):
    def fetch(j):
        return pltpu.make_async_copy(vals_hbm.at[j], vals.at[j], sems.at[j])

    others = [
        pltpu.make_async_copy(cols_hbm, cols, sems.at[r]),
        pltpu.make_async_copy(agg_hbm, agg, sems.at[r + 1]),
        pltpu.make_async_copy(inv_hbm, inv, sems.at[r + 2]),
    ]
    others[0].start()
    others[1].start()
    for j in range(r):
        fetch(j).start()
    others[2].start()

    def clear(j, carry):
        dense[rows(j, b), :] = jnp.zeros((b, (r + 2 * s) * b), BF16)
        return carry

    lax.fori_loop(0, r, clear, 0)
    others[0].wait()
    others[1].wait()
    zero = jnp.zeros((b, b), BF16)
    for j in range(r):
        own = slice(j * b, (j + 1) * b)
        block = pay[own, :]
        here = agg[j]
        for c in range(CA):
            placed[own, c * b : (c + 1) * b] = jnp.where(here == c, block, zero)
    odd = par[0]
    left = s * (1 - odd)

    def row(j, carry):
        fetch(j).wait()
        at = rows(j, b)
        for e in range(k):
            c = cols[j, e]
            c = jnp.where(c < r, c, jnp.where(c < r + s, c + left, c - left))
            dense[at, rows(c, b)] = vals[j, e]
        return carry

    lax.fori_loop(0, r, row, 0)
    others[2].wait()
    smooth(r, b, dense, slice(0, r * b), placed[...], inv, damp, p_own, placed)


def near_kernel(r, b, s, ghost, par, damp, dense, inv, pay, p_s, meta, placed):
    place_ghosts(r, b, s, ghost, 1 - par[0], pay, meta, placed)
    smooth(r, b, dense, slice(r * b, (r + s) * b), placed[...], inv, damp, p_s)


def far_kernel(r, b, s, w, ghost, par, damp, dense, inv, p_s, p_own, pay_s, pay_x, p_x, out_x, out_s, meta, near, placed):
    odd = par[0]
    place_ghosts(r, b, s, ghost, odd, pay_x, meta, placed)
    near[...] = pay_s[r * b :, :].astype(F32)
    wanted = (wanted_rows(r, s, 1 - odd, meta), wanted_rows(r, s, odd, near))
    smooth(r, b, dense, slice((r + s) * b, (r + 2 * s) * b), placed[...], inv, damp, p_x)
    for found, out in zip(wanted, (out_x, out_s)):
        for j in range(s):
            at = rows(found[j], b)
            to = slice(j * b, (j + 1) * b)
            out[to, :w] = p_s[at, :]
            out[to, w : 2 * w] = p_own[at, :]
            out[to, 2 * w :] = p_x[at, :]


def cross_kernel(parity, r, b, w, par, dense, p_s, p_own, p_x, *refs):
    y, gal, flipped = refs[-3:]

    @pl.when(par[0] == parity)
    def _():
        part_rows(r, b, w, dense, p_x, (p_s, p_own, p_x), y, gal, flipped)


def outer_kernel(parity, w, span, par, gal, y, far_s, out):
    @pl.when(par[0] == parity)
    def _():
        own = y.shape[1] - 2 * span
        by_s = dot(y[:, own : own + span], far_s[...])
        out[:, :w] = by_s[:, 2 * w :].astype(BF16)
        out[:, w : 2 * w] = (gal[:, :w] + by_s[:, w : 2 * w]).astype(BF16)
        out[:, 2 * w : 3 * w] = (gal[:, w : 2 * w] + by_s[:, :w]).astype(BF16)
        out[:, 3 * w : 4 * w] = gal[:, 2 * w :].astype(BF16)
        out[:, 4 * w :] = y[:, own + span :]


def flip(r, b, p, flipped):
    for j in range(r):
        at = slice(j * b, (j + 1) * b)
        flipped[:, at] = p[at, :].T


def part_rows(r, b, w, dense, p, parts, y, gal, flipped):
    flip(r, b, p, flipped)
    y[...] = dot(flipped[...], dense[...]).astype(BF16)
    for d, other in enumerate(parts):
        gal[:, d * w : (d + 1) * w] = dot(y[:, : r * b], other[...])


def rest_kernel(r, b, w, dense, p_s, p_own, p_x, y_s, gal_s, y_own, gal_own, flipped, flipped_own):
    parts = (p_s, p_own, p_x)
    part_rows(r, b, w, dense, p_s, parts, y_s, gal_s, flipped)
    part_rows(r, b, w, dense, p_own, parts, y_own, gal_own, flipped_own)


def galerkin_rows(w, span, gal, y, far_s, far_x):
    own = y.shape[1] - 2 * span
    by_s = dot(y[:, own : own + span], far_s[...])
    by_x = dot(y[:, own + span :], far_x[...])
    return (
        by_s[:, 2 * w :],
        gal[:, :w] + by_s[:, w : 2 * w],
        gal[:, w : 2 * w] + by_s[:, :w] + by_x[:, 2 * w :],
        gal[:, 2 * w :] + by_x[:, w : 2 * w],
        by_x[:, :w],
    )


def chip_kernel(w, span, gal, y, far_s, far_x, out):
    for c, value in enumerate(galerkin_rows(w, span, gal, y, far_s, far_x)):
        out[:, c * w : (c + 1) * w] = value.astype(BF16)


def inner_kernel(w, span, gal, y, far_s, far_x, from_s, out):
    mine = galerkin_rows(w, span, gal, y, far_s, far_x)
    for u in range(-3, 4):
        total = mine[2 - u] if abs(u) < 3 else jnp.zeros((w, w), F32)
        if 0 <= 1 + u < 5:
            total = total + from_s[:, (1 + u) * w : (2 + u) * w].astype(F32)
        out[:, (3 - u) * w : (4 - u) * w] = total


def final_kernel(w, par, mine, sent_x, from_odd, from_even, out_hbm, out, sems):
    def finish(sign, from_x):
        back = dot(from_x[:, 4 * w :], sent_x[...])
        copies = []
        for u in (3, 2, -3, -2, -1, 0, 1):
            total = mine[:, (3 - u) * w : (4 - u) * w]
            if 0 <= 3 + u < 4:
                total = total + from_x[:, (3 + u) * w : (4 + u) * w].astype(F32)
            if abs(u) < 2:
                total = total + back[:, (1 - u) * w : (2 - u) * w]
            out[u + 3, :, :] = total.astype(BF16)
            place = out_hbm.at[:, (3 + sign * u) * w : (4 + sign * u) * w]
            copies.append(pltpu.make_async_copy(out.at[u + 3], place, sems.at[u + 3]))
            copies[-1].start()
        for copy in copies:
            copy.wait()

    @pl.when(par[0] == 0)
    def _():
        finish(1, from_odd)

    @pl.when(par[0] == 1)
    def _():
        finish(-1, from_even)


def swap(x, route):
    return lax.ppermute(x, AXES, route)


def shards(block_values, block_columns, tentative, inverse_diagonal, aggregate, ghost_rows, damping):
    r, k = block_columns.shape
    b = tentative.shape[1]
    s = ghost_rows.shape[2]
    w = CA * b
    span = s * b
    devices = lax.axis_size(AXES)
    chip = [(i, i ^ 1) for i in range(devices) if i ^ 1 < devices]
    up = [(i, i + 1) for i in range(1, devices - 1, 2)]
    down = [(j, i) for i, j in up]
    _, dev = (lax.axis_index(a) for a in AXES)
    par = (dev & 1).astype(jnp.int32).reshape(1)
    tent = tentative.reshape(r * b, b)
    inv = inverse_diagonal.reshape(r * b, b)
    dma = pltpu.SemaphoreType.DMA
    total = (r + 2 * s) * b

    (pay,) = call(
        functools.partial(pack_kernel, r, b, s), (aggregate, ghost_rows, tent), "hhh",
        [((r * b + META, b), BF16)],
        scratch=[SMEM((r,), jnp.int32), SMEM((1, 2, s), jnp.int32), dma((3,))], limit=2 << 20,
    )
    pay_x = swap(pay, up + down)
    pay_s = swap(pay, chip)
    dense, inv, p_own = call(
        functools.partial(own_kernel, r, k, b, s),
        (par, damping, aggregate, block_columns, block_values, inv, pay), "sshhhhv",
        [((r * b, total), BF16), ((r * b, b), BF16), ((r * b, w), BF16)],
        scratch=[
            SMEM((r,), jnp.int32), SMEM((r, k), jnp.int32), VMEM((r, k, b, b), BF16), VMEM((r * b, w), BF16),
            dma((r + 3,)),
        ],
        flops=2 * r * b * r * b * w, limit=24 << 20,
    )
    (p_s,) = call(
        functools.partial(near_kernel, r, b, s), (ghost_rows, par, damping, dense, inv, pay_s), "sssvvv",
        [((r * b, w), BF16)], scratch=[VMEM((META, b), F32), VMEM((span, w), BF16)],
        flops=2 * r * b * span * w, limit=24 << 20,
    )
    p_x, out_x, out_s = call(
        functools.partial(far_kernel, r, b, s, w),
        (ghost_rows, par, damping, dense, inv, p_s, p_own, pay_s, pay_x), "sssvvvvvv",
        [((r * b, w), BF16), ((span, 3 * w), BF16), ((span, 3 * w), BF16)],
        scratch=[VMEM((META, b), F32), VMEM((META, b), F32), VMEM((span, w), BF16)],
        flops=2 * r * b * span * w, limit=24 << 20,
    )
    far_x = swap(out_x, up + down)
    far_s = swap(out_s, chip)
    shapes = [((w, total), BF16), ((w, 3 * w), F32)]
    scratch = [VMEM((w, r * b), BF16)]
    flops = 2 * r * b * r * b * 2 * w
    ready = (par, dense, p_s, p_own, p_x)

    def outer(parity, gal, y):
        return call(
            functools.partial(outer_kernel, parity, w, span), (par, gal, y, far_s), "svvv",
            [((w, 4 * w + span), BF16)], flops=2 * w * span * 3 * w, limit=16 << 20,
        )[0]

    y_x, gal_x = call(
        functools.partial(cross_kernel, 1, r, b, w), ready, "svvvv",
        shapes, scratch=scratch, flops=flops, limit=24 << 20,
    )
    from_odd = swap(outer(1, gal_x, y_x), up)
    y_x, gal_x = call(
        functools.partial(cross_kernel, 0, r, b, w), ready + (y_x, gal_x), "svvvvvv",
        shapes, scratch=scratch, flops=flops, limit=24 << 20, aliases={5: 0, 6: 1},
    )
    from_even = swap(outer(0, gal_x, y_x), down)
    y_s, gal_s, y_own, gal_own = call(
        functools.partial(rest_kernel, r, b, w), (dense, p_s, p_own, p_x), "vvvv",
        shapes + shapes, scratch=scratch + scratch, flops=2 * flops, limit=24 << 20,
    )
    (sum_s,) = call(
        functools.partial(chip_kernel, w, span), (gal_s, y_s, far_s, far_x), "vvvv",
        [((w, 5 * w), BF16)], flops=4 * w * span * 3 * w, limit=16 << 20,
    )
    from_s = swap(sum_s, chip)
    (mine,) = call(
        functools.partial(inner_kernel, w, span), (gal_own, y_own, far_s, far_x, from_s), "vvvvv",
        [((w, 7 * w), F32)], flops=4 * w * span * 3 * w, limit=16 << 20,
    )
    (out,) = call(
        functools.partial(final_kernel, w), (par, mine, out_x, from_odd, from_even), "svvvv",
        [((w, 7 * w), BF16)], scratch=[VMEM((7, w, w), BF16), dma((7,))],
        flops=2 * w * span * 3 * w, limit=16 << 20, out_space=pltpu.HBM,
    )
    return out.reshape(CA, b, 7 * w)


def solution(mesh):
    return jax.shard_map(
        shards,
        mesh=mesh,
        in_specs=(
            P(AXES, None, None, None),
            P(AXES, None),
            P(AXES, None, None),
            P(AXES, None, None),
            P(AXES),
            P(AXES, None, None),
            P(),
        ),
        out_specs=P(AXES, None, None),
        check_vma=False,
    )
```

```python
import functools

import jax
import jax.numpy as jnp
from jax import lax
from jax.experimental import pallas as pl
from jax.experimental.pallas import tpu as pltpu
from jax.sharding import PartitionSpec as P

CA = 2
META = 32
AXES = ("grp", "dev")
VMEM = pltpu.VMEM
SMEM = pltpu.SMEM
F32 = jnp.float32
BF16 = jnp.bfloat16


SPACES = {"v": VMEM, "s": SMEM, "h": pltpu.HBM}


def call(kernel, args, spaces, outs, scratch=(), flops=1, limit=None, aliases=None, out_space=VMEM):
    nbytes = sum(a.size * a.dtype.itemsize for a in args)
    in_specs = [pl.BlockSpec(memory_space=SPACES[c]) for c in spaces]
    return pl.pallas_call(
        kernel,
        out_shape=[jax.ShapeDtypeStruct(*o) for o in outs],
        in_specs=in_specs,
        out_specs=[pl.BlockSpec(memory_space=out_space) for _ in outs],
        scratch_shapes=list(scratch),
        input_output_aliases=aliases or {},
        cost_estimate=pl.CostEstimate(flops=flops, bytes_accessed=nbytes, transcendentals=0),
        compiler_params=pltpu.CompilerParams(vmem_limit_bytes=limit),
    )(*[pltpu.with_memory_space_constraint(a, pltpu.HBM) if c == "h" else a for a, c in zip(args, spaces)])


def rows(index, size):
    return pl.ds(pl.multiple_of(index * size, size), size)


def dot(a, b):
    return jnp.dot(a, b, preferred_element_type=F32)


def pack_kernel(r, b, s, agg_hbm, ghost_hbm, tent_hbm, out, agg, ghost, sems):
    copies = [
        pltpu.make_async_copy(agg_hbm, agg, sems.at[0]),
        pltpu.make_async_copy(ghost_hbm, ghost, sems.at[1]),
        pltpu.make_async_copy(tent_hbm, out.at[: r * b, :], sems.at[2]),
    ]
    for copy in copies:
        copy.start()
    copies[0].wait()
    copies[1].wait()
    sub = lax.broadcasted_iota(jnp.int32, (META, b), 0)
    meta = jnp.zeros((META, b), F32)
    for j in range(r):
        meta = jnp.where(sub == j, agg[j].astype(F32), meta)
    for side in range(2):
        for j in range(s):
            meta = jnp.where(sub == 16 + 8 * side + j, ghost[0, side, j].astype(F32), meta)
    out[r * b :, :] = meta.astype(BF16)
    copies[2].wait()


def smooth(r, b, dense, cols, placed, inv, damp, half, target, base=None):
    step = 4
    for t in range(r // step):
        at = slice(t * step * b, (t + 1) * step * b)
        half[at, :] = dot(dense[at, cols], placed[...]).astype(BF16)
    factor = -damp[0:1, :]
    for j in range(r):
        at = slice(j * b, (j + 1) * b)
        value = factor * dot(inv[at, :], half[at, :])
        if base is not None:
            value = base[at, :].astype(F32) + value
        target[at, :] = value.astype(BF16)


def place_ghosts(r, b, s, ghost, mine, pay, meta, placed):
    meta[...] = pay[r * b :, :].astype(F32)
    for j in range(s):
        row = jnp.clip(ghost[0, mine, j], 0, r - 1)
        block = pay[rows(row, b), :]
        here = jnp.broadcast_to(meta[pl.ds(row, 1), :], (b, b))
        for c in range(CA):
            placed[j * b : (j + 1) * b, c * b : (c + 1) * b] = jnp.where(here == c, block.astype(F32), 0.0).astype(BF16)


def wanted_rows(r, s, theirs, meta):
    found = []
    for j in range(s):
        value = jnp.max(meta[pl.ds(16 + 8 * theirs + j, 1), :])
        found.append(jnp.clip(value.astype(jnp.int32), 0, r - 1))
    return found


def own_kernel(
    r, k, b, s, index, damp_in, agg_hbm, cols_hbm, inv_hbm, vals_hbm, pay,
    dense, inv, p_own, damp, agg, cols, vals, placed, half, sems,
):
    def fetch(j):
        return pltpu.make_async_copy(vals_hbm.at[j], vals.at[j], sems.at[3 + j])

    pairs = ((cols_hbm, cols), (agg_hbm, agg), (inv_hbm, inv))
    others = [pltpu.make_async_copy(src, dst, sems.at[i]) for i, (src, dst) in enumerate(pairs)]
    for copy in others[:2]:
        copy.start()
    for j in range(r):
        fetch(j).start()
    others[2].start()

    def clear(j, carry):
        dense[rows(j, b), :] = jnp.zeros((b, (r + 2 * s) * b), BF16)
        return carry

    lax.fori_loop(0, r, clear, 0)
    for copy in others[:2]:
        copy.wait()
    damp[...] = jnp.full(damp.shape, damp_in[0], F32)
    zero = jnp.zeros((b, b), BF16)
    for j in range(r):
        own = slice(j * b, (j + 1) * b)
        block = pay[own, :]
        here = agg[j]
        for c in range(CA):
            placed[own, c * b : (c + 1) * b] = jnp.where(here == c, block, zero)
    odd = (index[0] & 1)
    left = s * (1 - odd)

    def row(j, carry):
        fetch(j).wait()
        at = rows(j, b)
        for e in range(k):
            c = cols[j, e]
            c = jnp.where(c < r, c, jnp.where(c < r + s, c + left, c - left))
            dense[at, rows(c, b)] = vals[j, e]
        return carry

    lax.fori_loop(0, r, row, 0)
    others[2].wait()
    smooth(r, b, dense, slice(0, r * b), placed, inv, damp, half, p_own, placed)


def near_kernel(r, b, s, ghost, index, damp, dense, inv, pay, p_s, meta, placed, half):
    place_ghosts(r, b, s, ghost, 1 - (index[0] & 1), pay, meta, placed)
    smooth(r, b, dense, slice(r * b, (r + s) * b), placed, inv, damp, half, p_s)


def far_kernel(r, b, s, w, ghost, index, damp, dense, inv, p_s, p_own, pay_s, pay_x, p_x, out_x, out_s, meta, near, placed, half):
    odd = (index[0] & 1)
    place_ghosts(r, b, s, ghost, odd, pay_x, meta, placed)
    near[...] = pay_s[r * b :, :].astype(F32)
    wanted = (wanted_rows(r, s, 1 - odd, meta), wanted_rows(r, s, odd, near))
    smooth(r, b, dense, slice((r + s) * b, (r + 2 * s) * b), placed, inv, damp, half, p_x)
    for found, out in zip(wanted, (out_x, out_s)):
        for j in range(s):
            at = rows(found[j], b)
            to = slice(j * b, (j + 1) * b)
            out[to, :w] = p_s[at, :]
            out[to, w : 2 * w] = p_own[at, :]
            out[to, 2 * w :] = p_x[at, :]


def cross_kernel(ahead, group, r, b, w, index, dense, p_s, p_own, p_x, *refs):
    y, gal, flipped = refs[-3:]

    opens = (lax.rem(index[0], group) == 0) & (index[0] > 0)

    @pl.when(opens if ahead else jnp.logical_not(opens))
    def _():
        part_rows(r, b, w, dense, p_x, (p_s, p_own, p_x), y, gal, flipped)


def outer_kernel(w, span, gal, y, far_s, out):
    own = y.shape[1] - 2 * span
    by_s = dot(y[:, own : own + span], far_s[...])
    out[:, :w] = by_s[:, 2 * w :].astype(BF16)
    out[:, w : 2 * w] = (gal[:, :w] + by_s[:, w : 2 * w]).astype(BF16)
    out[:, 2 * w : 3 * w] = (gal[:, w : 2 * w] + by_s[:, :w]).astype(BF16)
    out[:, 3 * w : 4 * w] = gal[:, 2 * w :].astype(BF16)
    out[:, 4 * w :] = y[:, own + span :]


def flip(r, b, p, flipped):
    for j in range(r):
        at = slice(j * b, (j + 1) * b)
        flipped[:, at] = p[at, :].T


def part_rows(r, b, w, dense, p, parts, y, gal, flipped):
    flip(r, b, p, flipped)
    y[...] = dot(flipped[...], dense[...]).astype(BF16)
    for d, other in enumerate(parts):
        gal[:, d * w : (d + 1) * w] = dot(y[:, : r * b], other[...])


def rest_kernel(r, b, w, dense, p_s, p_own, p_x, y_s, gal_s, y_own, gal_own, flipped, flipped_own):
    parts = (p_s, p_own, p_x)
    part_rows(r, b, w, dense, p_s, parts, y_s, gal_s, flipped)
    part_rows(r, b, w, dense, p_own, parts, y_own, gal_own, flipped_own)


def galerkin_rows(w, span, gal, y, far_s, far_x):
    own = y.shape[1] - 2 * span
    by_s = dot(y[:, own : own + span], far_s[...])
    by_x = dot(y[:, own + span :], far_x[...])
    return (
        by_s[:, 2 * w :],
        gal[:, :w] + by_s[:, w : 2 * w],
        gal[:, w : 2 * w] + by_s[:, :w] + by_x[:, 2 * w :],
        gal[:, 2 * w :] + by_x[:, w : 2 * w],
        by_x[:, :w],
    )


def chip_kernel(w, span, gal, y, far_s, far_x, out):
    for c, value in enumerate(galerkin_rows(w, span, gal, y, far_s, far_x)):
        out[:, c * w : (c + 1) * w] = value.astype(BF16)


def inner_kernel(w, span, gal, y, far_s, far_x, from_s, out):
    mine = galerkin_rows(w, span, gal, y, far_s, far_x)
    for u in range(-3, 4):
        total = mine[2 - u] if abs(u) < 3 else jnp.zeros((w, w), F32)
        if 0 <= 1 + u < 5:
            total = total + from_s[:, (1 + u) * w : (2 + u) * w].astype(F32)
        out[:, (3 - u) * w : (4 - u) * w] = total


def final_kernel(w, index, mine, sent_x, from_x, out_hbm, out, sems):
    sign = 1 - 2 * (index[0] & 1)
    back = dot(from_x[:, 4 * w :], sent_x[...])
    copies = []
    for u in (3, 2, -3, -2, -1, 0, 1):
        total = mine[:, (3 - u) * w : (4 - u) * w]
        if 0 <= 3 + u < 4:
            total = total + from_x[:, (3 + u) * w : (4 + u) * w].astype(F32)
        if abs(u) < 2:
            total = total + back[:, (1 - u) * w : (2 - u) * w]
        out[u + 3, :, :] = total.astype(BF16)
        copies.append(pltpu.make_async_copy(out.at[u + 3], out_hbm.at[:, rows(3 + sign * u, w)], sems.at[u + 3]))
        copies[-1].start()
    for copy in copies:
        copy.wait()


def swap(x, route):
    return lax.ppermute(x, AXES, route)


def shards(block_values, block_columns, tentative, inverse_diagonal, aggregate, ghost_rows, damping):
    r, k = block_columns.shape
    b = tentative.shape[1]
    s = ghost_rows.shape[2]
    w = CA * b
    span = s * b
    devices = lax.axis_size(AXES)
    chip = [(i, i ^ 1) for i in range(devices) if i ^ 1 < devices]
    cross = []
    for i in range(1, devices - 1, 2):
        cross += [(i, i + 1), (i + 1, i)]
    index = lax.axis_index(AXES).astype(jnp.int32).reshape(1)
    group = lax.axis_size(AXES[1])
    tent = tentative.reshape(r * b, b)
    inv = inverse_diagonal.reshape(r * b, b)
    dma = pltpu.SemaphoreType.DMA
    total = (r + 2 * s) * b

    (pay,) = call(
        functools.partial(pack_kernel, r, b, s), (aggregate, ghost_rows, tent), "hhh",
        [((r * b + META, b), BF16)],
        scratch=[SMEM((r,), jnp.int32), SMEM((1, 2, s), jnp.int32), dma((3,))], limit=2 << 20,
    )
    pay_x = swap(pay, cross)
    pay_s = swap(pay, chip)
    dense, inv, p_own, damp = call(
        functools.partial(own_kernel, r, k, b, s),
        (index, damping, aggregate, block_columns, inv, block_values, pay), "sshhhhv",
        [((r * b, total), BF16), ((r * b, b), BF16), ((r * b, w), BF16), ((8, w), F32)],
        scratch=[
            SMEM((r,), jnp.int32), SMEM((r, k), jnp.int32), VMEM((r, k, b, b), BF16),
            VMEM((r * b, w), BF16), VMEM((r * b, w), BF16), dma((r + 3,)),
        ],
        flops=2 * r * b * r * b * w, limit=24 << 20,
    )
    (p_s,) = call(
        functools.partial(near_kernel, r, b, s), (ghost_rows, index, damp, dense, inv, pay_s), "ssvvvv",
        [((r * b, w), BF16)], scratch=[VMEM((META, b), F32), VMEM((span, w), BF16), VMEM((r * b, w), BF16)],
        flops=2 * r * b * span * w, limit=24 << 20,
    )
    p_x, out_x, out_s = call(
        functools.partial(far_kernel, r, b, s, w),
        (ghost_rows, index, damp, dense, inv, p_s, p_own, pay_s, pay_x), "ssvvvvvvv",
        [((r * b, w), BF16), ((span, 3 * w), BF16), ((span, 3 * w), BF16)],
        scratch=[VMEM((META, b), F32), VMEM((META, b), F32), VMEM((span, w), BF16), VMEM((r * b, w), BF16)],
        flops=2 * r * b * span * w, limit=24 << 20,
    )
    far_x = swap(out_x, cross)
    far_s = swap(out_s, chip)
    shapes = [((w, total), BF16), ((w, 3 * w), F32)]
    scratch = [VMEM((w, r * b), BF16)]
    flops = 2 * r * b * r * b * 2 * w
    ready = (index, dense, p_s, p_own, p_x)
    y_x, gal_x = call(
        functools.partial(cross_kernel, True, group, r, b, w), ready, "svvvv",
        shapes, scratch=scratch, flops=flops, limit=24 << 20,
    )
    y_x, gal_x = call(
        functools.partial(cross_kernel, False, group, r, b, w), ready + (y_x, gal_x), "svvvvvv",
        shapes, scratch=scratch, flops=flops, limit=24 << 20, aliases={5: 0, 6: 1},
    )
    (sum_x,) = call(
        functools.partial(outer_kernel, w, span), (gal_x, y_x, far_s), "vvv",
        [((w, 4 * w + span), BF16)], flops=2 * w * span * 3 * w, limit=16 << 20,
    )
    from_x = swap(sum_x, cross)
    y_s, gal_s, y_own, gal_own = call(
        functools.partial(rest_kernel, r, b, w), (dense, p_s, p_own, p_x), "vvvv",
        shapes + shapes, scratch=scratch + scratch, flops=2 * flops, limit=24 << 20,
    )
    (sum_s,) = call(
        functools.partial(chip_kernel, w, span), (gal_s, y_s, far_s, far_x), "vvvv",
        [((w, 5 * w), BF16)], flops=4 * w * span * 3 * w, limit=16 << 20,
    )
    from_s = swap(sum_s, chip)
    (mine,) = call(
        functools.partial(inner_kernel, w, span), (gal_own, y_own, far_s, far_x, from_s), "vvvvv",
        [((w, 7 * w), F32)], flops=4 * w * span * 3 * w, limit=16 << 20,
    )
    (out,) = call(
        functools.partial(final_kernel, w), (index, mine, out_x, from_x), "svvv",
        [((w, 7 * w), BF16)], scratch=[VMEM((7, w, w), BF16), dma((7,))],
        flops=2 * w * span * 3 * w, limit=16 << 20, out_space=pltpu.HBM,
    )
    return out.reshape(CA, b, 7 * w)


def solution(mesh):
    return jax.shard_map(
        shards,
        mesh=mesh,
        in_specs=(
            P(AXES, None, None, None),
            P(AXES, None),
            P(AXES, None, None),
            P(AXES, None, None),
            P(AXES),
            P(AXES, None, None),
            P(),
        ),
        out_specs=P(AXES, None, None),
        check_vma=False,
    )
```

```python
import functools

import jax
import jax.numpy as jnp
from jax import lax
from jax.experimental import pallas as pl
from jax.experimental.pallas import tpu as pltpu
from jax.sharding import PartitionSpec as P

CA = 2
META = 32
AXES = ("grp", "dev")
VMEM = pltpu.VMEM
SMEM = pltpu.SMEM
F32 = jnp.float32
BF16 = jnp.bfloat16


SPACES = {"v": VMEM, "s": SMEM, "h": pltpu.HBM}


def call(kernel, args, spaces, outs, scratch=(), flops=1, limit=None, aliases=None, out_space=VMEM):
    nbytes = sum(a.size * a.dtype.itemsize for a in args)
    in_specs = [pl.BlockSpec(memory_space=SPACES[c]) for c in spaces]
    return pl.pallas_call(
        kernel,
        out_shape=[jax.ShapeDtypeStruct(*o) for o in outs],
        in_specs=in_specs,
        out_specs=[pl.BlockSpec(memory_space=out_space) for _ in outs],
        scratch_shapes=list(scratch),
        input_output_aliases=aliases or {},
        cost_estimate=pl.CostEstimate(flops=flops, bytes_accessed=nbytes, transcendentals=0),
        compiler_params=pltpu.CompilerParams(vmem_limit_bytes=limit),
    )(*[pltpu.with_memory_space_constraint(a, pltpu.HBM) if c == "h" else a for a, c in zip(args, spaces)])


def rows(index, size):
    return pl.ds(pl.multiple_of(index * size, size), size)


def dot(a, b):
    return jnp.dot(a, b, preferred_element_type=F32)


def pack_kernel(
    group, r, b, s, index, agg_hbm, ghost_hbm, tent_hbm, vals_hbm, out, dense, vals, agg, ghost, sems, fetch_sems
):
    copies = [
        pltpu.make_async_copy(agg_hbm, agg, sems.at[0]),
        pltpu.make_async_copy(ghost_hbm, ghost, sems.at[1]),
        pltpu.make_async_copy(tent_hbm, out.at[: r * b, :], sems.at[2]),
    ]
    for copy in copies:
        copy.start()
    copies[0].wait()
    copies[1].wait()
    sub = lax.broadcasted_iota(jnp.int32, (META, b), 0)
    meta = jnp.zeros((META, b), F32)
    for j in range(r):
        meta = jnp.where(sub == j, agg[j].astype(F32), meta)
    for side in range(2):
        for j in range(s):
            meta = jnp.where(sub == 16 + 8 * side + j, ghost[0, side, j].astype(F32), meta)
    out[r * b :, :] = meta.astype(BF16)

    @pl.when(opens_group(index, group))
    def _():
        fetches = fetch_blocks(r, vals_hbm, vals, fetch_sems)
        clear_rows(r, b, dense)
        for copy in fetches:
            copy.wait()

    copies[2].wait()


def opens_group(index, group):
    return (lax.rem(index[0], group) == 0) & (index[0] > 0)


def fetch_blocks(r, vals_hbm, vals, sems):
    copies = [pltpu.make_async_copy(vals_hbm.at[j], vals.at[j], sems.at[j]) for j in range(r)]
    for copy in copies:
        copy.start()
    return copies


def clear_rows(r, b, dense):
    def clear(j, carry):
        dense[rows(j, b), :] = jnp.zeros((b, dense.shape[1]), BF16)
        return carry

    lax.fori_loop(0, r, clear, 0)


def smooth(r, b, dense, cols, placed, inv, damp, half, target, base=None):
    step = 4
    for t in range(r // step):
        at = slice(t * step * b, (t + 1) * step * b)
        half[at, :] = dot(dense[at, cols], placed[...]).astype(BF16)
    factor = -damp[0:1, :]
    for j in range(r):
        at = slice(j * b, (j + 1) * b)
        value = factor * dot(inv[at, :], half[at, :])
        if base is not None:
            value = base[at, :].astype(F32) + value
        target[at, :] = value.astype(BF16)


def place_ghosts(r, b, s, ghost, mine, pay, meta, placed):
    meta[...] = pay[r * b :, :].astype(F32)
    for j in range(s):
        row = jnp.clip(ghost[0, mine, j], 0, r - 1)
        block = pay[rows(row, b), :]
        here = jnp.broadcast_to(meta[pl.ds(row, 1), :], (b, b))
        for c in range(CA):
            placed[j * b : (j + 1) * b, c * b : (c + 1) * b] = jnp.where(here == c, block.astype(F32), 0.0).astype(BF16)


def wanted_rows(r, s, theirs, meta):
    found = []
    for j in range(s):
        value = jnp.max(meta[pl.ds(16 + 8 * theirs + j, 1), :])
        found.append(jnp.clip(value.astype(jnp.int32), 0, r - 1))
    return found


def own_kernel(
    group, r, k, b, s, index, damp_in, agg_hbm, cols_hbm, inv_hbm, vals_hbm, pay, dense_in, vals_in,
    dense, vals, inv, p_own, damp, agg, cols, placed, half, sems, fetch_sems,
):
    pairs = ((cols_hbm, cols), (agg_hbm, agg), (inv_hbm, inv))
    others = [pltpu.make_async_copy(src, dst, sems.at[i]) for i, (src, dst) in enumerate(pairs)]
    for copy in others:
        copy.start()

    @pl.when(jnp.logical_not(opens_group(index, group)))
    def _():
        fetches = fetch_blocks(r, vals_hbm, vals, fetch_sems)
        clear_rows(r, b, dense)
        for copy in fetches:
            copy.wait()

    for copy in others[:2]:
        copy.wait()
    damp[...] = jnp.full(damp.shape, damp_in[0], F32)
    zero = jnp.zeros((b, b), BF16)
    for j in range(r):
        own = slice(j * b, (j + 1) * b)
        block = pay[own, :]
        here = agg[j]
        for c in range(CA):
            placed[own, c * b : (c + 1) * b] = jnp.where(here == c, block, zero)
    odd = (index[0] & 1)
    left = s * (1 - odd)

    def row(j, carry):
        at = rows(j, b)
        for e in range(k):
            c = cols[j, e]
            c = jnp.where(c < r, c, jnp.where(c < r + s, c + left, c - left))
            dense[at, rows(c, b)] = vals[j, e]
        return carry

    lax.fori_loop(0, r, row, 0)
    others[2].wait()
    smooth(r, b, dense, slice(0, r * b), placed, inv, damp, half, p_own, placed)


def near_kernel(r, b, s, ghost, index, damp, dense, inv, pay, p_s, meta, placed, half):
    place_ghosts(r, b, s, ghost, 1 - (index[0] & 1), pay, meta, placed)
    smooth(r, b, dense, slice(r * b, (r + s) * b), placed, inv, damp, half, p_s)


def far_kernel(r, b, s, w, ghost, index, damp, dense, inv, p_s, p_own, pay_s, pay_x, p_x, out_x, out_s, meta, near, placed, half):
    odd = (index[0] & 1)
    place_ghosts(r, b, s, ghost, odd, pay_x, meta, placed)
    near[...] = pay_s[r * b :, :].astype(F32)
    wanted = (wanted_rows(r, s, 1 - odd, meta), wanted_rows(r, s, odd, near))
    smooth(r, b, dense, slice((r + s) * b, (r + 2 * s) * b), placed, inv, damp, half, p_x)
    for found, out in zip(wanted, (out_x, out_s)):
        for j in range(s):
            at = rows(found[j], b)
            to = slice(j * b, (j + 1) * b)
            out[to, :w] = p_s[at, :]
            out[to, w : 2 * w] = p_own[at, :]
            out[to, 2 * w :] = p_x[at, :]


def cross_kernel(ahead, group, r, b, w, index, dense, p_s, p_own, p_x, *refs):
    y, gal, flipped = refs[-3:]

    opens = opens_group(index, group)

    @pl.when(opens if ahead else jnp.logical_not(opens))
    def _():
        part_rows(r, b, w, dense, p_x, (p_s, p_own, p_x), y, gal, flipped)


def outer_kernel(w, span, gal, y, far_s, out):
    own = y.shape[1] - 2 * span
    by_s = dot(y[:, own : own + span], far_s[...])
    out[:, :w] = by_s[:, 2 * w :].astype(BF16)
    out[:, w : 2 * w] = (gal[:, :w] + by_s[:, w : 2 * w]).astype(BF16)
    out[:, 2 * w : 3 * w] = (gal[:, w : 2 * w] + by_s[:, :w]).astype(BF16)
    out[:, 3 * w : 4 * w] = gal[:, 2 * w :].astype(BF16)
    out[:, 4 * w :] = y[:, own + span :]


def flip(r, b, p, flipped):
    for j in range(r):
        at = slice(j * b, (j + 1) * b)
        flipped[:, at] = p[at, :].T


def part_rows(r, b, w, dense, p, parts, y, gal, flipped):
    flip(r, b, p, flipped)
    y[...] = dot(flipped[...], dense[...]).astype(BF16)
    for d, other in enumerate(parts):
        gal[:, d * w : (d + 1) * w] = dot(y[:, : r * b], other[...])


def rest_kernel(which, r, b, w, dense, p_s, p_own, p_x, y, gal, flipped):
    parts = (p_s, p_own, p_x)
    part_rows(r, b, w, dense, parts[which], parts, y, gal, flipped)


def galerkin_rows(w, span, gal, y, far_s, far_x):
    own = y.shape[1] - 2 * span
    by_s = dot(y[:, own : own + span], far_s[...])
    by_x = dot(y[:, own + span :], far_x[...])
    return (
        by_s[:, 2 * w :],
        gal[:, :w] + by_s[:, w : 2 * w],
        gal[:, w : 2 * w] + by_s[:, :w] + by_x[:, 2 * w :],
        gal[:, 2 * w :] + by_x[:, w : 2 * w],
        by_x[:, :w],
    )


def chip_kernel(w, span, gal, y, far_s, far_x, out):
    for c, value in enumerate(galerkin_rows(w, span, gal, y, far_s, far_x)):
        out[:, c * w : (c + 1) * w] = value.astype(BF16)


def inner_kernel(w, span, gal, y, far_s, far_x, from_s, out):
    mine = galerkin_rows(w, span, gal, y, far_s, far_x)
    for u in range(-3, 4):
        total = mine[2 - u] if abs(u) < 3 else jnp.zeros((w, w), F32)
        if 0 <= 1 + u < 5:
            total = total + from_s[:, (1 + u) * w : (2 + u) * w].astype(F32)
        out[:, (3 - u) * w : (4 - u) * w] = total


def final_kernel(w, index, mine, sent_x, from_x, out_hbm, out, sems):
    sign = 1 - 2 * (index[0] & 1)
    back = dot(from_x[:, 4 * w :], sent_x[...])
    copies = []
    for u in (3, 2, -3, -2, -1, 0, 1):
        total = mine[:, (3 - u) * w : (4 - u) * w]
        if 0 <= 3 + u < 4:
            total = total + from_x[:, (3 + u) * w : (4 + u) * w].astype(F32)
        if abs(u) < 2:
            total = total + back[:, (1 - u) * w : (2 - u) * w]
        out[u + 3, :, :] = total.astype(BF16)
        copies.append(pltpu.make_async_copy(out.at[u + 3], out_hbm.at[:, rows(3 + sign * u, w)], sems.at[u + 3]))
        copies[-1].start()
    for copy in copies:
        copy.wait()


def swap(x, route):
    return lax.ppermute(x, AXES, route)


def shards(block_values, block_columns, tentative, inverse_diagonal, aggregate, ghost_rows, damping):
    r, k = block_columns.shape
    b = tentative.shape[1]
    s = ghost_rows.shape[2]
    w = CA * b
    span = s * b
    devices = lax.axis_size(AXES)
    chip = [(i, i ^ 1) for i in range(devices) if i ^ 1 < devices]
    cross = []
    for i in range(1, devices - 1, 2):
        cross += [(i, i + 1), (i + 1, i)]
    index = lax.axis_index(AXES).astype(jnp.int32).reshape(1)
    group = lax.axis_size(AXES[1])
    tent = tentative.reshape(r * b, b)
    inv = inverse_diagonal.reshape(r * b, b)
    dma = pltpu.SemaphoreType.DMA
    total = (r + 2 * s) * b

    dense_shape, vals_shape = ((r * b, total), BF16), ((r, k, b, b), BF16)
    pay, dense, vals = call(
        functools.partial(pack_kernel, group, r, b, s), (index, aggregate, ghost_rows, tent, block_values), "shhhh",
        [((r * b + META, b), BF16), dense_shape, vals_shape],
        scratch=[SMEM((r,), jnp.int32), SMEM((1, 2, s), jnp.int32), dma((3,)), dma((r,))], limit=12 << 20,
    )
    pay_x = swap(pay, cross)
    pay_s = swap(pay, chip)
    dense, _, inv, p_own, damp = call(
        functools.partial(own_kernel, group, r, k, b, s),
        (index, damping, aggregate, block_columns, inv, block_values, pay, dense, vals), "sshhhhvvv",
        [dense_shape, vals_shape, ((r * b, b), BF16), ((r * b, w), BF16), ((8, w), F32)],
        scratch=[
            SMEM((r,), jnp.int32), SMEM((r, k), jnp.int32), VMEM((r * b, w), BF16), VMEM((r * b, w), BF16),
            dma((3,)), dma((r,)),
        ],
        flops=2 * r * b * r * b * w, limit=24 << 20, aliases={7: 0, 8: 1},
    )
    (p_s,) = call(
        functools.partial(near_kernel, r, b, s), (ghost_rows, index, damp, dense, inv, pay_s), "ssvvvv",
        [((r * b, w), BF16)], scratch=[VMEM((META, b), F32), VMEM((span, w), BF16), VMEM((r * b, w), BF16)],
        flops=2 * r * b * span * w, limit=24 << 20,
    )
    p_x, out_x, out_s = call(
        functools.partial(far_kernel, r, b, s, w),
        (ghost_rows, index, damp, dense, inv, p_s, p_own, pay_s, pay_x), "ssvvvvvvv",
        [((r * b, w), BF16), ((span, 3 * w), BF16), ((span, 3 * w), BF16)],
        scratch=[VMEM((META, b), F32), VMEM((META, b), F32), VMEM((span, w), BF16), VMEM((r * b, w), BF16)],
        flops=2 * r * b * span * w, limit=24 << 20,
    )
    far_x = swap(out_x, cross)
    far_s = swap(out_s, chip)
    shapes = [((w, total), BF16), ((w, 3 * w), F32)]
    scratch = [VMEM((w, r * b), BF16)]
    flops = 2 * r * b * r * b * 2 * w
    ready = (index, dense, p_s, p_own, p_x)
    y_x, gal_x = call(
        functools.partial(cross_kernel, True, group, r, b, w), ready, "svvvv",
        shapes, scratch=scratch, flops=flops, limit=24 << 20,
    )
    y_x, gal_x = call(
        functools.partial(cross_kernel, False, group, r, b, w), ready + (y_x, gal_x), "svvvvvv",
        shapes, scratch=scratch, flops=flops, limit=24 << 20, aliases={5: 0, 6: 1},
    )
    (sum_x,) = call(
        functools.partial(outer_kernel, w, span), (gal_x, y_x, far_s), "vvv",
        [((w, 4 * w + span), BF16)], flops=2 * w * span * 3 * w, limit=16 << 20,
    )
    from_x = swap(sum_x, cross)

    def rest(which):
        return call(
            functools.partial(rest_kernel, which, r, b, w), (dense, p_s, p_own, p_x), "vvvv",
            shapes, scratch=scratch, flops=flops, limit=24 << 20,
        )

    y_s, gal_s = rest(0)
    (sum_s,) = call(
        functools.partial(chip_kernel, w, span), (gal_s, y_s, far_s, far_x), "vvvv",
        [((w, 5 * w), BF16)], flops=4 * w * span * 3 * w, limit=16 << 20,
    )
    from_s = swap(sum_s, chip)
    y_own, gal_own = rest(1)
    (mine,) = call(
        functools.partial(inner_kernel, w, span), (gal_own, y_own, far_s, far_x, from_s), "vvvvv",
        [((w, 7 * w), F32)], flops=4 * w * span * 3 * w, limit=16 << 20,
    )
    (out,) = call(
        functools.partial(final_kernel, w), (index, mine, out_x, from_x), "svvv",
        [((w, 7 * w), BF16)], scratch=[VMEM((7, w, w), BF16), dma((7,))],
        flops=2 * w * span * 3 * w, limit=16 << 20, out_space=pltpu.HBM,
    )
    return out.reshape(CA, b, 7 * w)


def solution(mesh):
    return jax.shard_map(
        shards,
        mesh=mesh,
        in_specs=(
            P(AXES, None, None, None),
            P(AXES, None),
            P(AXES, None, None),
            P(AXES, None, None),
            P(AXES),
            P(AXES, None, None),
            P(),
        ),
        out_specs=P(AXES, None, None),
        check_vma=False,
    )
```

```python
import functools

import jax
import jax.numpy as jnp
from jax import lax
from jax.experimental import pallas as pl
from jax.experimental.pallas import tpu as pltpu
from jax.sharding import PartitionSpec as P

CA = 2
META = 32
AXES = ("grp", "dev")
VMEM = pltpu.VMEM
SMEM = pltpu.SMEM
F32 = jnp.float32
BF16 = jnp.bfloat16


SPACES = {"v": VMEM, "s": SMEM, "h": pltpu.HBM}


def call(kernel, args, spaces, outs, scratch=(), flops=1, limit=None, aliases=None, out_space=VMEM):
    nbytes = sum(a.size * a.dtype.itemsize for a in args)
    in_specs = [pl.BlockSpec(memory_space=SPACES[c]) for c in spaces]
    return pl.pallas_call(
        kernel,
        out_shape=[jax.ShapeDtypeStruct(*o) for o in outs],
        in_specs=in_specs,
        out_specs=[pl.BlockSpec(memory_space=out_space) for _ in outs],
        scratch_shapes=list(scratch),
        input_output_aliases=aliases or {},
        cost_estimate=pl.CostEstimate(flops=flops, bytes_accessed=nbytes, transcendentals=0),
        compiler_params=pltpu.CompilerParams(vmem_limit_bytes=limit),
    )(*[pltpu.with_memory_space_constraint(a, pltpu.HBM) if c == "h" else a for a, c in zip(args, spaces)])


def rows(index, size):
    return pl.ds(pl.multiple_of(index * size, size), size)


def dot(a, b):
    return jnp.dot(a, b, preferred_element_type=F32)


def pack_kernel(r, b, s, agg_hbm, ghost_hbm, tent_hbm, out, agg, ghost, sems):
    copies = [
        pltpu.make_async_copy(agg_hbm, agg, sems.at[0]),
        pltpu.make_async_copy(ghost_hbm, ghost, sems.at[1]),
        pltpu.make_async_copy(tent_hbm, out.at[: r * b, :], sems.at[2]),
    ]
    for copy in copies:
        copy.start()
    copies[0].wait()
    copies[1].wait()
    sub = lax.broadcasted_iota(jnp.int32, (META, b), 0)
    meta = jnp.zeros((META, b), F32)
    for j in range(r):
        meta = jnp.where(sub == j, agg[j].astype(F32), meta)
    for side in range(2):
        for j in range(s):
            meta = jnp.where(sub == 16 + 8 * side + j, ghost[0, side, j].astype(F32), meta)
    out[r * b :, :] = meta.astype(BF16)
    copies[2].wait()


def smooth(r, b, dense, cols, placed, inv, damp, half, target, base=None, before=None):
    step = 4
    for t in range(r // step):
        if before is not None:
            before(range(t * step, (t + 1) * step))
        at = slice(t * step * b, (t + 1) * step * b)
        half[at, :] = dot(dense[at, cols], placed[...]).astype(BF16)
    factor = -damp[0:1, :]
    for j in range(r):
        at = slice(j * b, (j + 1) * b)
        value = factor * dot(inv[at, :], half[at, :])
        if base is not None:
            value = base[at, :].astype(F32) + value
        target[at, :] = value.astype(BF16)


def place_ghosts(r, b, s, ghost, mine, pay, meta, placed):
    meta[...] = pay[r * b :, :].astype(F32)
    for j in range(s):
        row = jnp.clip(ghost[0, mine, j], 0, r - 1)
        block = pay[rows(row, b), :]
        here = jnp.broadcast_to(meta[pl.ds(row, 1), :], (b, b))
        for c in range(CA):
            placed[j * b : (j + 1) * b, c * b : (c + 1) * b] = jnp.where(here == c, block.astype(F32), 0.0).astype(BF16)


def wanted_rows(r, s, theirs, meta):
    found = []
    for j in range(s):
        value = jnp.max(meta[pl.ds(16 + 8 * theirs + j, 1), :])
        found.append(jnp.clip(value.astype(jnp.int32), 0, r - 1))
    return found


def own_kernel(
    r, k, b, s, index, damp_in, agg_hbm, cols_hbm, inv_hbm, vals_hbm, pay,
    dense, inv, p_own, damp, agg, cols, placed, half, sems, block_sems,
):
    pairs = ((cols_hbm, cols), (agg_hbm, agg), (inv_hbm, inv))
    others = [pltpu.make_async_copy(src, dst, sems.at[i]) for i, (src, dst) in enumerate(pairs)]
    for copy in others:
        copy.start()

    def clear(j, carry):
        dense[rows(j, b), :] = jnp.zeros((b, (r + 2 * s) * b), BF16)
        return carry

    lax.fori_loop(0, r, clear, 0)
    others[0].wait()
    left = s * (1 - (index[0] & 1))

    def fetch(j, e):
        c = cols[j, e]
        c = jnp.where(c < r, c, jnp.where(c < r + s, c + left, c - left))
        return pltpu.make_async_copy(vals_hbm.at[j, e], dense.at[rows(j, b), rows(c, b)], block_sems.at[j, e])

    def start(j, carry):
        for e in range(k):
            fetch(j, e).start()
        return carry

    def wait(found):
        def finish(j, carry):
            for e in range(k):
                fetch(j, e).wait()
            return carry

        lax.fori_loop(found.start, found.stop, finish, 0)

    lax.fori_loop(0, r, start, 0)
    others[1].wait()
    damp[...] = jnp.full(damp.shape, damp_in[0], F32)
    zero = jnp.zeros((b, b), BF16)
    for j in range(r):
        own = slice(j * b, (j + 1) * b)
        block = pay[own, :]
        here = agg[j]
        for c in range(CA):
            placed[own, c * b : (c + 1) * b] = jnp.where(here == c, block, zero)
    others[2].wait()
    smooth(r, b, dense, slice(0, r * b), placed, inv, damp, half, p_own, placed, wait)


def near_kernel(r, b, s, ghost, index, damp, dense, inv, pay, p_s, meta, placed, half):
    place_ghosts(r, b, s, ghost, 1 - (index[0] & 1), pay, meta, placed)
    smooth(r, b, dense, slice(r * b, (r + s) * b), placed, inv, damp, half, p_s)


def far_kernel(r, b, s, w, ghost, index, damp, dense, inv, p_s, p_own, pay_s, pay_x, p_x, out_x, out_s, meta, near, placed, half):
    odd = (index[0] & 1)
    place_ghosts(r, b, s, ghost, odd, pay_x, meta, placed)
    near[...] = pay_s[r * b :, :].astype(F32)
    wanted = (wanted_rows(r, s, 1 - odd, meta), wanted_rows(r, s, odd, near))
    smooth(r, b, dense, slice((r + s) * b, (r + 2 * s) * b), placed, inv, damp, half, p_x)
    for found, out in zip(wanted, (out_x, out_s)):
        for j in range(s):
            at = rows(found[j], b)
            to = slice(j * b, (j + 1) * b)
            out[to, :w] = p_s[at, :]
            out[to, w : 2 * w] = p_own[at, :]
            out[to, 2 * w :] = p_x[at, :]


def cross_kernel(ahead, group, r, b, w, index, dense, p_s, p_own, p_x, *refs):
    y, gal, flipped = refs[-3:]

    opens = (lax.rem(index[0], group) == 0) & (index[0] > 0)

    @pl.when(opens if ahead else jnp.logical_not(opens))
    def _():
        part_rows(r, b, w, dense, p_x, (p_s, p_own, p_x), y, gal, flipped)


def outer_kernel(w, span, gal, y, far_s, out):
    own = y.shape[1] - 2 * span
    by_s = dot(y[:, own : own + span], far_s[...])
    out[:, :w] = by_s[:, 2 * w :].astype(BF16)
    out[:, w : 2 * w] = (gal[:, :w] + by_s[:, w : 2 * w]).astype(BF16)
    out[:, 2 * w : 3 * w] = (gal[:, w : 2 * w] + by_s[:, :w]).astype(BF16)
    out[:, 3 * w : 4 * w] = gal[:, 2 * w :].astype(BF16)
    out[:, 4 * w :] = y[:, own + span :]


def flip(r, b, p, flipped):
    for j in range(r):
        at = slice(j * b, (j + 1) * b)
        flipped[:, at] = p[at, :].T


def part_rows(r, b, w, dense, p, parts, y, gal, flipped):
    flip(r, b, p, flipped)
    y[...] = dot(flipped[...], dense[...]).astype(BF16)
    for d, other in enumerate(parts):
        gal[:, d * w : (d + 1) * w] = dot(y[:, : r * b], other[...])


def rest_kernel(which, r, b, w, dense, p_s, p_own, p_x, y, gal, flipped):
    parts = (p_s, p_own, p_x)
    part_rows(r, b, w, dense, parts[which], parts, y, gal, flipped)


def galerkin_rows(w, span, gal, y, far_s, far_x):
    own = y.shape[1] - 2 * span
    by_s = dot(y[:, own : own + span], far_s[...])
    by_x = dot(y[:, own + span :], far_x[...])
    return (
        by_s[:, 2 * w :],
        gal[:, :w] + by_s[:, w : 2 * w],
        gal[:, w : 2 * w] + by_s[:, :w] + by_x[:, 2 * w :],
        gal[:, 2 * w :] + by_x[:, w : 2 * w],
        by_x[:, :w],
    )


def chip_kernel(w, span, gal, y, far_s, far_x, out):
    for c, value in enumerate(galerkin_rows(w, span, gal, y, far_s, far_x)):
        out[:, c * w : (c + 1) * w] = value.astype(BF16)


def inner_kernel(w, span, gal, y, far_s, far_x, from_s, out):
    mine = galerkin_rows(w, span, gal, y, far_s, far_x)
    for u in range(-3, 4):
        total = mine[2 - u] if abs(u) < 3 else jnp.zeros((w, w), F32)
        if 0 <= 1 + u < 5:
            total = total + from_s[:, (1 + u) * w : (2 + u) * w].astype(F32)
        out[:, (3 - u) * w : (4 - u) * w] = total


def final_kernel(w, index, mine, sent_x, from_x, out_hbm, out, sems):
    sign = 1 - 2 * (index[0] & 1)
    back = dot(from_x[:, 4 * w :], sent_x[...])
    copies = []
    for u in (3, 2, -3, -2, -1, 0, 1):
        total = mine[:, (3 - u) * w : (4 - u) * w]
        if 0 <= 3 + u < 4:
            total = total + from_x[:, (3 + u) * w : (4 + u) * w].astype(F32)
        if abs(u) < 2:
            total = total + back[:, (1 - u) * w : (2 - u) * w]
        out[u + 3, :, :] = total.astype(BF16)
        copies.append(pltpu.make_async_copy(out.at[u + 3], out_hbm.at[:, rows(3 + sign * u, w)], sems.at[u + 3]))
        copies[-1].start()
    for copy in copies:
        copy.wait()


def swap(x, route):
    return lax.ppermute(x, AXES, route)


def shards(block_values, block_columns, tentative, inverse_diagonal, aggregate, ghost_rows, damping):
    r, k = block_columns.shape
    b = tentative.shape[1]
    s = ghost_rows.shape[2]
    w = CA * b
    span = s * b
    devices = lax.axis_size(AXES)
    chip = [(i, i ^ 1) for i in range(devices) if i ^ 1 < devices]
    cross = []
    for i in range(1, devices - 1, 2):
        cross += [(i, i + 1), (i + 1, i)]
    index = lax.axis_index(AXES).astype(jnp.int32).reshape(1)
    group = lax.axis_size(AXES[1])
    tent = tentative.reshape(r * b, b)
    inv = inverse_diagonal.reshape(r * b, b)
    dma = pltpu.SemaphoreType.DMA
    total = (r + 2 * s) * b

    (pay,) = call(
        functools.partial(pack_kernel, r, b, s), (aggregate, ghost_rows, tent), "hhh",
        [((r * b + META, b), BF16)],
        scratch=[SMEM((r,), jnp.int32), SMEM((1, 2, s), jnp.int32), dma((3,))], limit=2 << 20,
    )
    pay_x = swap(pay, cross)
    pay_s = swap(pay, chip)
    dense, inv, p_own, damp = call(
        functools.partial(own_kernel, r, k, b, s),
        (index, damping, aggregate, block_columns, inv, block_values, pay), "sshhhhv",
        [((r * b, total), BF16), ((r * b, b), BF16), ((r * b, w), BF16), ((8, w), F32)],
        scratch=[
            SMEM((r,), jnp.int32), SMEM((r, k), jnp.int32), VMEM((r * b, w), BF16), VMEM((r * b, w), BF16),
            dma((3,)), dma((r, k)),
        ],
        flops=2 * r * b * r * b * w, limit=24 << 20,
    )
    (p_s,) = call(
        functools.partial(near_kernel, r, b, s), (ghost_rows, index, damp, dense, inv, pay_s), "ssvvvv",
        [((r * b, w), BF16)], scratch=[VMEM((META, b), F32), VMEM((span, w), BF16), VMEM((r * b, w), BF16)],
        flops=2 * r * b * span * w, limit=24 << 20,
    )
    p_x, out_x, out_s = call(
        functools.partial(far_kernel, r, b, s, w),
        (ghost_rows, index, damp, dense, inv, p_s, p_own, pay_s, pay_x), "ssvvvvvvv",
        [((r * b, w), BF16), ((span, 3 * w), BF16), ((span, 3 * w), BF16)],
        scratch=[VMEM((META, b), F32), VMEM((META, b), F32), VMEM((span, w), BF16), VMEM((r * b, w), BF16)],
        flops=2 * r * b * span * w, limit=24 << 20,
    )
    far_x = swap(out_x, cross)
    far_s = swap(out_s, chip)
    shapes = [((w, total), BF16), ((w, 3 * w), F32)]
    scratch = [VMEM((w, r * b), BF16)]
    flops = 2 * r * b * r * b * 2 * w
    ready = (index, dense, p_s, p_own, p_x)
    y_x, gal_x = call(
        functools.partial(cross_kernel, True, group, r, b, w), ready, "svvvv",
        shapes, scratch=scratch, flops=flops, limit=24 << 20,
    )
    y_x, gal_x = call(
        functools.partial(cross_kernel, False, group, r, b, w), ready + (y_x, gal_x), "svvvvvv",
        shapes, scratch=scratch, flops=flops, limit=24 << 20, aliases={5: 0, 6: 1},
    )
    (sum_x,) = call(
        functools.partial(outer_kernel, w, span), (gal_x, y_x, far_s), "vvv",
        [((w, 4 * w + span), BF16)], flops=2 * w * span * 3 * w, limit=16 << 20,
    )
    from_x = swap(sum_x, cross)

    def rest(which):
        return call(
            functools.partial(rest_kernel, which, r, b, w), (dense, p_s, p_own, p_x), "vvvv",
            shapes, scratch=scratch, flops=flops, limit=24 << 20,
        )

    y_s, gal_s = rest(0)
    (sum_s,) = call(
        functools.partial(chip_kernel, w, span), (gal_s, y_s, far_s, far_x), "vvvv",
        [((w, 5 * w), BF16)], flops=4 * w * span * 3 * w, limit=16 << 20,
    )
    from_s = swap(sum_s, chip)
    y_own, gal_own = rest(1)
    (mine,) = call(
        functools.partial(inner_kernel, w, span), (gal_own, y_own, far_s, far_x, from_s), "vvvvv",
        [((w, 7 * w), F32)], flops=4 * w * span * 3 * w, limit=16 << 20,
    )
    (out,) = call(
        functools.partial(final_kernel, w), (index, mine, out_x, from_x), "svvv",
        [((w, 7 * w), BF16)], scratch=[VMEM((7, w, w), BF16), dma((7,))],
        flops=2 * w * span * 3 * w, limit=16 << 20, out_space=pltpu.HBM,
    )
    return out.reshape(CA, b, 7 * w)


def solution(mesh):
    return jax.shard_map(
        shards,
        mesh=mesh,
        in_specs=(
            P(AXES, None, None, None),
            P(AXES, None),
            P(AXES, None, None),
            P(AXES, None, None),
            P(AXES),
            P(AXES, None, None),
            P(),
        ),
        out_specs=P(AXES, None, None),
        check_vma=False,
    )
```

```python
import functools

import jax
import jax.numpy as jnp
from jax import lax
from jax.experimental import pallas as pl
from jax.experimental.pallas import tpu as pltpu
from jax.sharding import PartitionSpec as P

CA = 2
META = 32
AXES = ("grp", "dev")
VMEM = pltpu.VMEM
SMEM = pltpu.SMEM
F32 = jnp.float32
BF16 = jnp.bfloat16


SPACES = {"v": VMEM, "s": SMEM, "h": pltpu.HBM}


def call(kernel, args, spaces, outs, scratch=(), flops=1, limit=None, aliases=None, out_space=VMEM):
    nbytes = sum(a.size * a.dtype.itemsize for a in args)
    in_specs = [pl.BlockSpec(memory_space=SPACES[c]) for c in spaces]
    return pl.pallas_call(
        kernel,
        out_shape=[jax.ShapeDtypeStruct(*o) for o in outs],
        in_specs=in_specs,
        out_specs=[pl.BlockSpec(memory_space=out_space) for _ in outs],
        scratch_shapes=list(scratch),
        input_output_aliases=aliases or {},
        cost_estimate=pl.CostEstimate(flops=flops, bytes_accessed=nbytes, transcendentals=0),
        compiler_params=pltpu.CompilerParams(vmem_limit_bytes=limit),
    )(*[pltpu.with_memory_space_constraint(a, pltpu.HBM) if c == "h" else a for a, c in zip(args, spaces)])


def rows(index, size):
    return pl.ds(pl.multiple_of(index * size, size), size)


def dot(a, b):
    return jnp.dot(a, b, preferred_element_type=F32)


def pack_kernel(r, b, s, agg_hbm, ghost_hbm, tent_hbm, out, agg, ghost, sems):
    copies = [
        pltpu.make_async_copy(agg_hbm, agg, sems.at[0]),
        pltpu.make_async_copy(ghost_hbm, ghost, sems.at[1]),
        pltpu.make_async_copy(tent_hbm, out.at[: r * b, :], sems.at[2]),
    ]
    for copy in copies:
        copy.start()
    copies[0].wait()
    copies[1].wait()
    sub = lax.broadcasted_iota(jnp.int32, (META, b), 0)
    meta = jnp.zeros((META, b), F32)
    for j in range(r):
        meta = jnp.where(sub == j, agg[j].astype(F32), meta)
    for side in range(2):
        for j in range(s):
            meta = jnp.where(sub == 16 + 8 * side + j, ghost[0, side, j].astype(F32), meta)
    out[r * b :, :] = meta.astype(BF16)
    copies[2].wait()


def smooth(r, b, dense, cols, placed, inv, damp, half, target, base=None):
    step = 4
    for t in range(r // step):
        at = slice(t * step * b, (t + 1) * step * b)
        half[at, :] = dot(dense[at, cols], placed[...]).astype(BF16)
    factor = -damp[0:1, :]
    for j in range(r):
        at = slice(j * b, (j + 1) * b)
        value = factor * dot(inv[at, :], half[at, :])
        if base is not None:
            value = base[at, :].astype(F32) + value
        target[at, :] = value.astype(BF16)


def place_ghosts(r, b, s, ghost, mine, pay, meta, placed):
    meta[...] = pay[r * b :, :].astype(F32)
    for j in range(s):
        row = jnp.clip(ghost[0, mine, j], 0, r - 1)
        block = pay[rows(row, b), :]
        here = jnp.broadcast_to(meta[pl.ds(row, 1), :], (b, b))
        for c in range(CA):
            placed[j * b : (j + 1) * b, c * b : (c + 1) * b] = jnp.where(here == c, block.astype(F32), 0.0).astype(BF16)


def wanted_rows(r, s, theirs, meta):
    found = []
    for j in range(s):
        value = jnp.max(meta[pl.ds(16 + 8 * theirs + j, 1), :])
        found.append(jnp.clip(value.astype(jnp.int32), 0, r - 1))
    return found


def own_kernel(
    r, k, b, s, index, damp_in, agg_hbm, cols_hbm, inv_hbm, vals_hbm, pay,
    dense, inv, p_own, damp, agg, cols, vals, placed, half, sems,
):
    def fetch(j):
        return pltpu.make_async_copy(vals_hbm.at[j], vals.at[j], sems.at[3 + j])

    pairs = ((cols_hbm, cols), (agg_hbm, agg), (inv_hbm, inv))
    others = [pltpu.make_async_copy(src, dst, sems.at[i]) for i, (src, dst) in enumerate(pairs)]
    for copy in others[:2]:
        copy.start()
    for j in range(r):
        fetch(j).start()
    others[2].start()

    def clear(j, carry):
        dense[rows(j, b), :] = jnp.zeros((b, (r + 2 * s) * b), BF16)
        return carry

    lax.fori_loop(0, r, clear, 0)
    for copy in others[:2]:
        copy.wait()
    damp[...] = jnp.full(damp.shape, damp_in[0], F32)
    zero = jnp.zeros((b, b), BF16)
    for j in range(r):
        own = slice(j * b, (j + 1) * b)
        block = pay[own, :]
        here = agg[j]
        for c in range(CA):
            placed[own, c * b : (c + 1) * b] = jnp.where(here == c, block, zero)
    odd = (index[0] & 1)
    left = s * (1 - odd)

    def row(j, carry):
        fetch(j).wait()
        at = rows(j, b)
        for e in range(k):
            c = cols[j, e]
            c = jnp.where(c < r, c, jnp.where(c < r + s, c + left, c - left))
            dense[at, rows(c, b)] = vals[j, e]
        return carry

    lax.fori_loop(0, r, row, 0)
    others[2].wait()
    smooth(r, b, dense, slice(0, r * b), placed, inv, damp, half, p_own, placed)


def near_kernel(r, b, s, ghost, index, damp, dense, inv, pay, p_s, meta, placed, half):
    place_ghosts(r, b, s, ghost, 1 - (index[0] & 1), pay, meta, placed)
    smooth(r, b, dense, slice(r * b, (r + s) * b), placed, inv, damp, half, p_s)


def far_kernel(r, b, s, w, ghost, index, damp, dense, inv, p_s, p_own, pay_s, pay_x, p_x, out_x, out_s, meta, near, placed, half):
    odd = (index[0] & 1)
    place_ghosts(r, b, s, ghost, odd, pay_x, meta, placed)
    near[...] = pay_s[r * b :, :].astype(F32)
    wanted = (wanted_rows(r, s, 1 - odd, meta), wanted_rows(r, s, odd, near))
    smooth(r, b, dense, slice((r + s) * b, (r + 2 * s) * b), placed, inv, damp, half, p_x)
    for found, out in zip(wanted, (out_x, out_s)):
        for j in range(s):
            at = rows(found[j], b)
            to = slice(j * b, (j + 1) * b)
            out[to, :w] = p_s[at, :]
            out[to, w : 2 * w] = p_own[at, :]
            out[to, 2 * w :] = p_x[at, :]


def opens_group(index, group):
    return (lax.rem(index[0], group) == 0) & (index[0] > 0)


def ahead_kernel(group, r, b, index, dense, p_x, y, flipped):
    @pl.when(opens_group(index, group))
    def _():
        left_product(r, b, dense, p_x, y, flipped)


def cross_kernel(group, r, b, w, index, dense, p_s, p_own, p_x, y_in, y, gal, flipped):
    @pl.when(jnp.logical_not(opens_group(index, group)))
    def _():
        left_product(r, b, dense, p_x, y, flipped)

    right_product(r, b, w, (p_s, p_own, p_x), y, gal)


def outer_kernel(w, span, gal, y, far_s, out):
    own = y.shape[1] - 2 * span
    by_s = dot(y[:, own : own + span], far_s[...])
    out[:, :w] = by_s[:, 2 * w :].astype(BF16)
    out[:, w : 2 * w] = (gal[:, :w] + by_s[:, w : 2 * w]).astype(BF16)
    out[:, 2 * w : 3 * w] = (gal[:, w : 2 * w] + by_s[:, :w]).astype(BF16)
    out[:, 3 * w : 4 * w] = gal[:, 2 * w :].astype(BF16)
    out[:, 4 * w :] = y[:, own + span :]


def flip(r, b, p, flipped):
    for j in range(r):
        at = slice(j * b, (j + 1) * b)
        flipped[:, at] = p[at, :].T


def left_product(r, b, dense, p, y, flipped):
    flip(r, b, p, flipped)
    y[...] = dot(flipped[...], dense[...]).astype(BF16)


def right_product(r, b, w, parts, y, gal):
    for d, other in enumerate(parts):
        gal[:, d * w : (d + 1) * w] = dot(y[:, : r * b], other[...])


def rest_kernel(which, r, b, w, dense, p_s, p_own, p_x, y, gal, flipped):
    parts = (p_s, p_own, p_x)
    left_product(r, b, dense, parts[which], y, flipped)
    right_product(r, b, w, parts, y, gal)


def galerkin_rows(w, span, gal, y, far_s, far_x):
    own = y.shape[1] - 2 * span
    by_s = dot(y[:, own : own + span], far_s[...])
    by_x = dot(y[:, own + span :], far_x[...])
    return (
        by_s[:, 2 * w :],
        gal[:, :w] + by_s[:, w : 2 * w],
        gal[:, w : 2 * w] + by_s[:, :w] + by_x[:, 2 * w :],
        gal[:, 2 * w :] + by_x[:, w : 2 * w],
        by_x[:, :w],
    )


def chip_kernel(w, span, gal, y, far_s, far_x, out):
    for c, value in enumerate(galerkin_rows(w, span, gal, y, far_s, far_x)):
        out[:, c * w : (c + 1) * w] = value.astype(BF16)


def inner_kernel(w, span, gal, y, far_s, far_x, from_s, out):
    mine = galerkin_rows(w, span, gal, y, far_s, far_x)
    for u in range(-3, 4):
        total = mine[2 - u] if abs(u) < 3 else jnp.zeros((w, w), F32)
        if 0 <= 1 + u < 5:
            total = total + from_s[:, (1 + u) * w : (2 + u) * w].astype(F32)
        out[:, (3 - u) * w : (4 - u) * w] = total


def final_kernel(w, index, mine, sent_x, from_x, out_hbm, out, sems):
    sign = 1 - 2 * (index[0] & 1)
    back = dot(from_x[:, 4 * w :], sent_x[...])
    copies = []
    for u in (3, 2, -3, -2, -1, 0, 1):
        total = mine[:, (3 - u) * w : (4 - u) * w]
        if 0 <= 3 + u < 4:
            total = total + from_x[:, (3 + u) * w : (4 + u) * w].astype(F32)
        if abs(u) < 2:
            total = total + back[:, (1 - u) * w : (2 - u) * w]
        out[u + 3, :, :] = total.astype(BF16)
        copies.append(pltpu.make_async_copy(out.at[u + 3], out_hbm.at[:, rows(3 + sign * u, w)], sems.at[u + 3]))
        copies[-1].start()
    for copy in copies:
        copy.wait()


def swap(x, route):
    return lax.ppermute(x, AXES, route)


def shards(block_values, block_columns, tentative, inverse_diagonal, aggregate, ghost_rows, damping):
    r, k = block_columns.shape
    b = tentative.shape[1]
    s = ghost_rows.shape[2]
    w = CA * b
    span = s * b
    devices = lax.axis_size(AXES)
    chip = [(i, i ^ 1) for i in range(devices) if i ^ 1 < devices]
    cross = []
    for i in range(1, devices - 1, 2):
        cross += [(i, i + 1), (i + 1, i)]
    index = lax.axis_index(AXES).astype(jnp.int32).reshape(1)
    group = lax.axis_size(AXES[1])
    tent = tentative.reshape(r * b, b)
    inv = inverse_diagonal.reshape(r * b, b)
    dma = pltpu.SemaphoreType.DMA
    total = (r + 2 * s) * b

    (pay,) = call(
        functools.partial(pack_kernel, r, b, s), (aggregate, ghost_rows, tent), "hhh",
        [((r * b + META, b), BF16)],
        scratch=[SMEM((r,), jnp.int32), SMEM((1, 2, s), jnp.int32), dma((3,))], limit=2 << 20,
    )
    pay_x = swap(pay, cross)
    pay_s = swap(pay, chip)
    dense, inv, p_own, damp = call(
        functools.partial(own_kernel, r, k, b, s),
        (index, damping, aggregate, block_columns, inv, block_values, pay), "sshhhhv",
        [((r * b, total), BF16), ((r * b, b), BF16), ((r * b, w), BF16), ((8, w), F32)],
        scratch=[
            SMEM((r,), jnp.int32), SMEM((r, k), jnp.int32), VMEM((r, k, b, b), BF16),
            VMEM((r * b, w), BF16), VMEM((r * b, w), BF16), dma((r + 3,)),
        ],
        flops=2 * r * b * r * b * w, limit=24 << 20,
    )
    (p_s,) = call(
        functools.partial(near_kernel, r, b, s), (ghost_rows, index, damp, dense, inv, pay_s), "ssvvvv",
        [((r * b, w), BF16)], scratch=[VMEM((META, b), F32), VMEM((span, w), BF16), VMEM((r * b, w), BF16)],
        flops=2 * r * b * span * w, limit=24 << 20,
    )
    p_x, out_x, out_s = call(
        functools.partial(far_kernel, r, b, s, w),
        (ghost_rows, index, damp, dense, inv, p_s, p_own, pay_s, pay_x), "ssvvvvvvv",
        [((r * b, w), BF16), ((span, 3 * w), BF16), ((span, 3 * w), BF16)],
        scratch=[VMEM((META, b), F32), VMEM((META, b), F32), VMEM((span, w), BF16), VMEM((r * b, w), BF16)],
        flops=2 * r * b * span * w, limit=24 << 20,
    )
    far_x = swap(out_x, cross)
    far_s = swap(out_s, chip)
    shapes = [((w, total), BF16), ((w, 3 * w), F32)]
    scratch = [VMEM((w, r * b), BF16)]
    flops = 2 * r * b * r * b * 2 * w
    (y_x,) = call(
        functools.partial(ahead_kernel, group, r, b), (index, dense, p_x), "svv",
        shapes[:1], scratch=scratch, flops=flops, limit=24 << 20,
    )
    y_x, gal_x = call(
        functools.partial(cross_kernel, group, r, b, w), (index, dense, p_s, p_own, p_x, y_x), "svvvvv",
        shapes, scratch=scratch, flops=flops, limit=24 << 20, aliases={5: 0},
    )
    (sum_x,) = call(
        functools.partial(outer_kernel, w, span), (gal_x, y_x, far_s), "vvv",
        [((w, 4 * w + span), BF16)], flops=2 * w * span * 3 * w, limit=16 << 20,
    )
    from_x = swap(sum_x, cross)

    def rest(which):
        return call(
            functools.partial(rest_kernel, which, r, b, w), (dense, p_s, p_own, p_x), "vvvv",
            shapes, scratch=scratch, flops=flops, limit=24 << 20,
        )

    y_s, gal_s = rest(0)
    (sum_s,) = call(
        functools.partial(chip_kernel, w, span), (gal_s, y_s, far_s, far_x), "vvvv",
        [((w, 5 * w), BF16)], flops=4 * w * span * 3 * w, limit=16 << 20,
    )
    from_s = swap(sum_s, chip)
    y_own, gal_own = rest(1)
    (mine,) = call(
        functools.partial(inner_kernel, w, span), (gal_own, y_own, far_s, far_x, from_s), "vvvvv",
        [((w, 7 * w), F32)], flops=4 * w * span * 3 * w, limit=16 << 20,
    )
    (out,) = call(
        functools.partial(final_kernel, w), (index, mine, out_x, from_x), "svvv",
        [((w, 7 * w), BF16)], scratch=[VMEM((7, w, w), BF16), dma((7,))],
        flops=2 * w * span * 3 * w, limit=16 << 20, out_space=pltpu.HBM,
    )
    return out.reshape(CA, b, 7 * w)


def solution(mesh):
    return jax.shard_map(
        shards,
        mesh=mesh,
        in_specs=(
            P(AXES, None, None, None),
            P(AXES, None),
            P(AXES, None, None),
            P(AXES, None, None),
            P(AXES),
            P(AXES, None, None),
            P(),
        ),
        out_specs=P(AXES, None, None),
        check_vma=False,
    )
```

```python
import functools

import jax
import jax.numpy as jnp
from jax import lax
from jax.experimental import pallas as pl
from jax.experimental.pallas import tpu as pltpu
from jax.sharding import PartitionSpec as P

CA = 2
META = 32
AXES = ("grp", "dev")
VMEM = pltpu.VMEM
SMEM = pltpu.SMEM
F32 = jnp.float32
BF16 = jnp.bfloat16


SPACES = {"v": VMEM, "s": SMEM, "h": pltpu.HBM}


def call(kernel, args, spaces, outs, scratch=(), flops=1, limit=None, aliases=None, out_space=VMEM):
    nbytes = sum(a.size * a.dtype.itemsize for a in args)
    in_specs = [pl.BlockSpec(memory_space=SPACES[c]) for c in spaces]
    return pl.pallas_call(
        kernel,
        out_shape=[jax.ShapeDtypeStruct(*o) for o in outs],
        in_specs=in_specs,
        out_specs=[pl.BlockSpec(memory_space=out_space) for _ in outs],
        scratch_shapes=list(scratch),
        input_output_aliases=aliases or {},
        cost_estimate=pl.CostEstimate(flops=flops, bytes_accessed=nbytes, transcendentals=0),
        compiler_params=pltpu.CompilerParams(vmem_limit_bytes=limit),
    )(*[pltpu.with_memory_space_constraint(a, pltpu.HBM) if c == "h" else a for a, c in zip(args, spaces)])


def rows(index, size):
    return pl.ds(pl.multiple_of(index * size, size), size)


def dot(a, b):
    return jnp.dot(a, b, preferred_element_type=F32)


def pack_kernel(r, b, s, agg_hbm, ghost_hbm, tent_hbm, out, agg, ghost, sems):
    copies = [
        pltpu.make_async_copy(agg_hbm, agg, sems.at[0]),
        pltpu.make_async_copy(ghost_hbm, ghost, sems.at[1]),
        pltpu.make_async_copy(tent_hbm, out.at[: r * b, :], sems.at[2]),
    ]
    for copy in copies:
        copy.start()
    copies[0].wait()
    copies[1].wait()
    sub = lax.broadcasted_iota(jnp.int32, (META, b), 0)
    meta = jnp.zeros((META, b), F32)
    for j in range(r):
        meta = jnp.where(sub == j, agg[j].astype(F32), meta)
    for side in range(2):
        for j in range(s):
            meta = jnp.where(sub == 16 + 8 * side + j, ghost[0, side, j].astype(F32), meta)
    out[r * b :, :] = meta.astype(BF16)
    copies[2].wait()


def smooth(r, b, dense, cols, placed, inv, damp, half, target, base=None):
    step = 4
    for t in range(r // step):
        at = slice(t * step * b, (t + 1) * step * b)
        half[at, :] = dot(dense[at, cols], placed[...]).astype(BF16)
    factor = -damp[0:1, :]
    for j in range(r):
        at = slice(j * b, (j + 1) * b)
        value = factor * dot(inv[at, :], half[at, :])
        if base is not None:
            value = base[at, :].astype(F32) + value
        target[at, :] = value.astype(BF16)


def to_row(line, r):
    return jnp.clip(jnp.max(line).astype(jnp.int32), 0, r - 1)


def place_ghosts(r, b, s, ghost, mine, pay, meta, placed):
    meta[...] = pay[r * b :, :].astype(F32)
    line = ghost[0, pl.ds(mine, 1), :].astype(F32)
    lane = lax.broadcasted_iota(jnp.int32, line.shape, 1)
    for j in range(s):
        row = to_row(jnp.where(lane == j, line, 0.0), r)
        block = pay[rows(row, b), :]
        here = jnp.broadcast_to(meta[pl.ds(row, 1), :], (b, b))
        for c in range(CA):
            placed[j * b : (j + 1) * b, c * b : (c + 1) * b] = jnp.where(here == c, block.astype(F32), 0.0).astype(BF16)


def wanted_rows(r, s, theirs, meta):
    found = []
    for j in range(s):
        found.append(to_row(meta[pl.ds(16 + 8 * theirs + j, 1), :], r))
    return found


def own_kernel(
    r, k, b, s, index, damp_in, agg_hbm, cols_hbm, inv_hbm, vals_hbm, pay,
    dense, inv, p_own, damp, agg, cols, vals, placed, half, sems,
):
    def fetch(j):
        return pltpu.make_async_copy(vals_hbm.at[j], vals.at[j], sems.at[3 + j])

    pairs = ((cols_hbm, cols), (agg_hbm, agg), (inv_hbm, inv))
    others = [pltpu.make_async_copy(src, dst, sems.at[i]) for i, (src, dst) in enumerate(pairs)]
    for copy in others[:2]:
        copy.start()
    for j in range(r):
        fetch(j).start()
    others[2].start()

    def clear(j, carry):
        dense[rows(j, b), :] = jnp.zeros((b, (r + 2 * s) * b), BF16)
        return carry

    lax.fori_loop(0, r, clear, 0)
    for copy in others[:2]:
        copy.wait()
    damp[...] = jnp.full(damp.shape, damp_in[0], F32)
    zero = jnp.zeros((b, b), BF16)
    for j in range(r):
        own = slice(j * b, (j + 1) * b)
        block = pay[own, :]
        here = agg[j]
        for c in range(CA):
            placed[own, c * b : (c + 1) * b] = jnp.where(here == c, block, zero)
    odd = (index[0] & 1)
    left = s * (1 - odd)

    def row(j, carry):
        fetch(j).wait()
        at = rows(j, b)
        for e in range(k):
            c = cols[j, e]
            c = jnp.where(c < r, c, jnp.where(c < r + s, c + left, c - left))
            dense[at, rows(c, b)] = vals[j, e]
        return carry

    lax.fori_loop(0, r, row, 0)
    others[2].wait()
    smooth(r, b, dense, slice(0, r * b), placed, inv, damp, half, p_own, placed)


def near_kernel(r, b, s, ghost, index, damp, dense, inv, pay, p_s, meta, placed, half):
    place_ghosts(r, b, s, ghost, 1 - (index[0] & 1), pay, meta, placed)
    smooth(r, b, dense, slice(r * b, (r + s) * b), placed, inv, damp, half, p_s)


def far_kernel(r, b, s, w, ghost, index, damp, dense, inv, p_s, p_own, pay_s, pay_x, p_x, out_x, out_s, meta, near, placed, half):
    odd = (index[0] & 1)
    place_ghosts(r, b, s, ghost, odd, pay_x, meta, placed)
    near[...] = pay_s[r * b :, :].astype(F32)
    wanted = (wanted_rows(r, s, 1 - odd, meta), wanted_rows(r, s, odd, near))
    smooth(r, b, dense, slice((r + s) * b, (r + 2 * s) * b), placed, inv, damp, half, p_x)
    for found, out in zip(wanted, (out_x, out_s)):
        for j in range(s):
            at = rows(found[j], b)
            to = slice(j * b, (j + 1) * b)
            out[to, :w] = p_s[at, :]
            out[to, w : 2 * w] = p_own[at, :]
            out[to, 2 * w :] = p_x[at, :]


def opens_group(index, group):
    return (lax.rem(index[0], group) == 0) & (index[0] > 0)


def ahead_kernel(group, r, b, index, dense, p_x, y, flipped):
    @pl.when(opens_group(index, group))
    def _():
        left_product(r, b, dense, p_x, y, flipped)


def cross_kernel(group, r, b, w, index, dense, p_s, p_own, p_x, y_in, y, gal, flipped):
    @pl.when(jnp.logical_not(opens_group(index, group)))
    def _():
        left_product(r, b, dense, p_x, y, flipped)

    right_product(r, b, w, (p_s, p_own, p_x), y, gal)


def outer_kernel(w, span, gal, y, far_s, out):
    own = y.shape[1] - 2 * span
    by_s = dot(y[:, own : own + span], far_s[...])
    out[:, :w] = by_s[:, 2 * w :].astype(BF16)
    out[:, w : 2 * w] = (gal[:, :w] + by_s[:, w : 2 * w]).astype(BF16)
    out[:, 2 * w : 3 * w] = (gal[:, w : 2 * w] + by_s[:, :w]).astype(BF16)
    out[:, 3 * w : 4 * w] = gal[:, 2 * w :].astype(BF16)
    out[:, 4 * w :] = y[:, own + span :]


def flip(r, b, p, flipped):
    for j in range(r):
        at = slice(j * b, (j + 1) * b)
        flipped[:, at] = p[at, :].T


def left_product(r, b, dense, p, y, flipped):
    flip(r, b, p, flipped)
    y[...] = dot(flipped[...], dense[...]).astype(BF16)


def right_product(r, b, w, parts, y, gal):
    for d, other in enumerate(parts):
        gal[:, d * w : (d + 1) * w] = dot(y[:, : r * b], other[...])


def rest_kernel(which, r, b, w, dense, p_s, p_own, p_x, y, gal, flipped):
    parts = (p_s, p_own, p_x)
    left_product(r, b, dense, parts[which], y, flipped)
    right_product(r, b, w, parts, y, gal)


def galerkin_rows(w, span, gal, y, far_s, far_x):
    own = y.shape[1] - 2 * span
    by_s = dot(y[:, own : own + span], far_s[...])
    by_x = dot(y[:, own + span :], far_x[...])
    return (
        by_s[:, 2 * w :],
        gal[:, :w] + by_s[:, w : 2 * w],
        gal[:, w : 2 * w] + by_s[:, :w] + by_x[:, 2 * w :],
        gal[:, 2 * w :] + by_x[:, w : 2 * w],
        by_x[:, :w],
    )


def chip_kernel(w, span, gal, y, far_s, far_x, out):
    for c, value in enumerate(galerkin_rows(w, span, gal, y, far_s, far_x)):
        out[:, c * w : (c + 1) * w] = value.astype(BF16)


def inner_kernel(w, span, gal, y, far_s, far_x, from_s, out):
    mine = galerkin_rows(w, span, gal, y, far_s, far_x)
    for u in range(-3, 4):
        total = mine[2 - u] if abs(u) < 3 else jnp.zeros((w, w), F32)
        if 0 <= 1 + u < 5:
            total = total + from_s[:, (1 + u) * w : (2 + u) * w].astype(F32)
        out[:, (3 - u) * w : (4 - u) * w] = total


def final_kernel(w, index, mine, sent_x, from_x, out_hbm, out, sems):
    sign = 1 - 2 * (index[0] & 1)
    copies = []
    for u in (3, 2, -3, -2, -1, 0, 1):
        total = mine[:, (3 - u) * w : (4 - u) * w]
        if 0 <= 3 + u < 4:
            total = total + from_x[:, (3 + u) * w : (4 + u) * w].astype(F32)
        if abs(u) < 2:
            total = total + dot(from_x[:, 4 * w :], sent_x[:, (1 - u) * w : (2 - u) * w])
        out[u + 3, :, :] = total.astype(BF16)
        copies.append(pltpu.make_async_copy(out.at[u + 3], out_hbm.at[:, rows(3 + sign * u, w)], sems.at[u + 3]))
        copies[-1].start()
    for copy in copies:
        copy.wait()


def swap(x, route):
    return lax.ppermute(x, AXES, route)


def shards(block_values, block_columns, tentative, inverse_diagonal, aggregate, ghost_rows, damping):
    r, k = block_columns.shape
    b = tentative.shape[1]
    s = ghost_rows.shape[2]
    w = CA * b
    span = s * b
    devices = lax.axis_size(AXES)
    chip = [(i, i ^ 1) for i in range(devices) if i ^ 1 < devices]
    cross = []
    for i in range(1, devices - 1, 2):
        cross += [(i, i + 1), (i + 1, i)]
    index = lax.axis_index(AXES).astype(jnp.int32).reshape(1)
    group = lax.axis_size(AXES[1])
    tent = tentative.reshape(r * b, b)
    inv = inverse_diagonal.reshape(r * b, b)
    dma = pltpu.SemaphoreType.DMA
    total = (r + 2 * s) * b

    (pay,) = call(
        functools.partial(pack_kernel, r, b, s), (aggregate, ghost_rows, tent), "hhh",
        [((r * b + META, b), BF16)],
        scratch=[SMEM((r,), jnp.int32), SMEM((1, 2, s), jnp.int32), dma((3,))], limit=2 << 20,
    )
    pay_x = swap(pay, cross)
    pay_s = swap(pay, chip)
    dense, inv, p_own, damp = call(
        functools.partial(own_kernel, r, k, b, s),
        (index, damping, aggregate, block_columns, inv, block_values, pay), "sshhhhv",
        [((r * b, total), BF16), ((r * b, b), BF16), ((r * b, w), BF16), ((8, w), F32)],
        scratch=[
            SMEM((r,), jnp.int32), SMEM((r, k), jnp.int32), VMEM((r, k, b, b), BF16),
            VMEM((r * b, w), BF16), VMEM((r * b, w), BF16), dma((r + 3,)),
        ],
        flops=2 * r * b * r * b * w, limit=24 << 20,
    )
    (p_s,) = call(
        functools.partial(near_kernel, r, b, s), (ghost_rows, index, damp, dense, inv, pay_s), "vsvvvv",
        [((r * b, w), BF16)], scratch=[VMEM((META, b), F32), VMEM((span, w), BF16), VMEM((r * b, w), BF16)],
        flops=2 * r * b * span * w, limit=24 << 20,
    )
    p_x, out_x, out_s = call(
        functools.partial(far_kernel, r, b, s, w),
        (ghost_rows, index, damp, dense, inv, p_s, p_own, pay_s, pay_x), "vsvvvvvvv",
        [((r * b, w), BF16), ((span, 3 * w), BF16), ((span, 3 * w), BF16)],
        scratch=[VMEM((META, b), F32), VMEM((META, b), F32), VMEM((span, w), BF16), VMEM((r * b, w), BF16)],
        flops=2 * r * b * span * w, limit=24 << 20,
    )
    far_x = swap(out_x, cross)
    far_s = swap(out_s, chip)
    shapes = [((w, total), BF16), ((w, 3 * w), F32)]
    scratch = [VMEM((w, r * b), BF16)]
    flops = 2 * r * b * r * b * 2 * w
    (y_x,) = call(
        functools.partial(ahead_kernel, group, r, b), (index, dense, p_x), "svv",
        shapes[:1], scratch=scratch, flops=flops, limit=24 << 20,
    )
    y_x, gal_x = call(
        functools.partial(cross_kernel, group, r, b, w), (index, dense, p_s, p_own, p_x, y_x), "svvvvv",
        shapes, scratch=scratch, flops=flops, limit=24 << 20, aliases={5: 0},
    )
    (sum_x,) = call(
        functools.partial(outer_kernel, w, span), (gal_x, y_x, far_s), "vvv",
        [((w, 4 * w + span), BF16)], flops=2 * w * span * 3 * w, limit=16 << 20,
    )
    from_x = swap(sum_x, cross)

    def rest(which):
        return call(
            functools.partial(rest_kernel, which, r, b, w), (dense, p_s, p_own, p_x), "vvvv",
            shapes, scratch=scratch, flops=flops, limit=24 << 20,
        )

    y_s, gal_s = rest(0)
    (sum_s,) = call(
        functools.partial(chip_kernel, w, span), (gal_s, y_s, far_s, far_x), "vvvv",
        [((w, 5 * w), BF16)], flops=4 * w * span * 3 * w, limit=16 << 20,
    )
    from_s = swap(sum_s, chip)
    y_own, gal_own = rest(1)
    (mine,) = call(
        functools.partial(inner_kernel, w, span), (gal_own, y_own, far_s, far_x, from_s), "vvvvv",
        [((w, 7 * w), F32)], flops=4 * w * span * 3 * w, limit=16 << 20,
    )
    (out,) = call(
        functools.partial(final_kernel, w), (index, mine, out_x, from_x), "svvv",
        [((w, 7 * w), BF16)], scratch=[VMEM((7, w, w), BF16), dma((7,))],
        flops=2 * w * span * 3 * w, limit=16 << 20, out_space=pltpu.HBM,
    )
    return out.reshape(CA, b, 7 * w)


def solution(mesh):
    return jax.shard_map(
        shards,
        mesh=mesh,
        in_specs=(
            P(AXES, None, None, None),
            P(AXES, None),
            P(AXES, None, None),
            P(AXES, None, None),
            P(AXES),
            P(AXES, None, None),
            P(),
        ),
        out_specs=P(AXES, None, None),
        check_vma=False,
    )
```

```python
import functools

import jax
import jax.numpy as jnp
from jax import lax
from jax.experimental import pallas as pl
from jax.experimental.pallas import tpu as pltpu
from jax.sharding import PartitionSpec as P

CA = 2
META = 32
AXES = ("grp", "dev")
VMEM = pltpu.VMEM
SMEM = pltpu.SMEM
F32 = jnp.float32
BF16 = jnp.bfloat16


SPACES = {"v": VMEM, "s": SMEM, "h": pltpu.HBM}


def call(kernel, args, spaces, outs, scratch=(), flops=1, limit=None, aliases=None, out_space=VMEM):
    nbytes = sum(a.size * a.dtype.itemsize for a in args)
    in_specs = [pl.BlockSpec(memory_space=SPACES[c]) for c in spaces]
    return pl.pallas_call(
        kernel,
        out_shape=[jax.ShapeDtypeStruct(*o) for o in outs],
        in_specs=in_specs,
        out_specs=[pl.BlockSpec(memory_space=out_space) for _ in outs],
        scratch_shapes=list(scratch),
        input_output_aliases=aliases or {},
        cost_estimate=pl.CostEstimate(flops=flops, bytes_accessed=nbytes, transcendentals=0),
        compiler_params=pltpu.CompilerParams(vmem_limit_bytes=limit),
    )(*[pltpu.with_memory_space_constraint(a, pltpu.HBM) if c == "h" else a for a, c in zip(args, spaces)])


def rows(index, size):
    return pl.ds(pl.multiple_of(index * size, size), size)


def dot(a, b):
    return jnp.dot(a, b, preferred_element_type=F32)


def pack_kernel(r, b, s, agg_hbm, ghost_hbm, tent_hbm, out, agg, ghost, sems):
    copies = [
        pltpu.make_async_copy(agg_hbm, agg, sems.at[0]),
        pltpu.make_async_copy(ghost_hbm, ghost, sems.at[1]),
        pltpu.make_async_copy(tent_hbm, out.at[: r * b, :], sems.at[2]),
    ]
    for copy in copies:
        copy.start()
    copies[0].wait()
    copies[1].wait()
    sub = lax.broadcasted_iota(jnp.int32, (META, b), 0)
    meta = jnp.zeros((META, b), F32)
    for j in range(r):
        meta = jnp.where(sub == j, agg[j].astype(F32), meta)
    for side in range(2):
        for j in range(s):
            meta = jnp.where(sub == 16 + 8 * side + j, ghost[0, side, j].astype(F32), meta)
    out[r * b :, :] = meta.astype(BF16)
    copies[2].wait()


def smooth(r, b, dense, cols, placed, inv, damp, half, target, base=None):
    step = 4
    for t in range(r // step):
        at = slice(t * step * b, (t + 1) * step * b)
        half[at, :] = dot(dense[at, cols], placed[...]).astype(BF16)
    factor = -damp[0:1, :]
    for j in range(r):
        at = slice(j * b, (j + 1) * b)
        value = factor * dot(inv[at, :], half[at, :])
        if base is not None:
            value = base[at, :].astype(F32) + value
        target[at, :] = value.astype(BF16)


def to_row(line, r):
    return jnp.clip(jnp.max(line).astype(jnp.int32), 0, r - 1)


def place_ghosts(r, b, s, ghost, mine, pay, meta, placed):
    meta[...] = pay[r * b :, :].astype(F32)
    line = ghost[0, pl.ds(mine, 1), :].astype(F32)
    lane = lax.broadcasted_iota(jnp.int32, line.shape, 1)
    for j in range(s):
        row = to_row(jnp.where(lane == j, line, 0.0), r)
        block = pay[rows(row, b), :]
        here = jnp.broadcast_to(meta[pl.ds(row, 1), :], (b, b))
        for c in range(CA):
            placed[j * b : (j + 1) * b, c * b : (c + 1) * b] = jnp.where(here == c, block.astype(F32), 0.0).astype(BF16)


def wanted_rows(r, s, theirs, meta):
    found = []
    for j in range(s):
        found.append(to_row(meta[pl.ds(16 + 8 * theirs + j, 1), :], r))
    return found


def own_kernel(
    r, k, b, s, index, damp_in, agg_hbm, cols_hbm, inv_hbm, vals_hbm, pay,
    dense, inv, p_own, damp, agg, cols, vals, placed, half, sems,
):
    def fetch(j):
        return pltpu.make_async_copy(vals_hbm.at[j], vals.at[j], sems.at[3 + j])

    pairs = ((cols_hbm, cols), (agg_hbm, agg), (inv_hbm, inv))
    others = [pltpu.make_async_copy(src, dst, sems.at[i]) for i, (src, dst) in enumerate(pairs)]
    for copy in others[:2]:
        copy.start()
    for j in range(r):
        fetch(j).start()
    others[2].start()

    def clear(j, carry):
        dense[rows(j, b), :] = jnp.zeros((b, (r + 2 * s) * b), BF16)
        return carry

    lax.fori_loop(0, r, clear, 0)
    for copy in others[:2]:
        copy.wait()
    damp[...] = jnp.full(damp.shape, damp_in[0], F32)
    zero = jnp.zeros((b, b), BF16)
    for j in range(r):
        own = slice(j * b, (j + 1) * b)
        block = pay[own, :]
        here = agg[j]
        for c in range(CA):
            placed[own, c * b : (c + 1) * b] = jnp.where(here == c, block, zero)
    odd = (index[0] & 1)
    left = s * (1 - odd)

    def row(j, carry):
        fetch(j).wait()
        at = rows(j, b)
        for e in range(k):
            c = cols[j, e]
            c = jnp.where(c < r, c, jnp.where(c < r + s, c + left, c - left))
            dense[at, rows(c, b)] = vals[j, e]
        return carry

    lax.fori_loop(0, r, row, 0)
    others[2].wait()
    smooth(r, b, dense, slice(0, r * b), placed, inv, damp, half, p_own, placed)


def near_kernel(r, b, s, ghost, index, damp, dense, inv, pay, p_s, meta, placed, half):
    place_ghosts(r, b, s, ghost, 1 - (index[0] & 1), pay, meta, placed)
    smooth(r, b, dense, slice(r * b, (r + s) * b), placed, inv, damp, half, p_s)


def far_kernel(r, b, s, w, ghost, index, damp, dense, inv, p_s, p_own, pay_s, pay_x, p_x, out_x, out_s, meta, near, placed, half):
    odd = (index[0] & 1)
    place_ghosts(r, b, s, ghost, odd, pay_x, meta, placed)
    near[...] = pay_s[r * b :, :].astype(F32)
    wanted = (wanted_rows(r, s, 1 - odd, meta), wanted_rows(r, s, odd, near))
    smooth(r, b, dense, slice((r + s) * b, (r + 2 * s) * b), placed, inv, damp, half, p_x)
    for found, out in zip(wanted, (out_x, out_s)):
        for j in range(s):
            at = rows(found[j], b)
            to = slice(j * b, (j + 1) * b)
            out[to, :w] = p_s[at, :]
            out[to, w : 2 * w] = p_own[at, :]
            out[to, 2 * w :] = p_x[at, :]


def opens_group(index, group):
    return (lax.rem(index[0], group) == 0) & (index[0] > 0)


def ahead_kernel(group, r, b, w, index, dense, p_s, p_x, y, gal, flipped):
    @pl.when(opens_group(index, group))
    def _():
        left_product(r, b, dense, p_x, y, flipped)
        right_product(r, b, w, (p_s,), y, gal)


def cross_kernel(group, r, b, w, index, dense, p_s, p_own, p_x, y_in, gal_in, y, gal, flipped):
    @pl.when(jnp.logical_not(opens_group(index, group)))
    def _():
        left_product(r, b, dense, p_x, y, flipped)
        right_product(r, b, w, (p_s,), y, gal)

    right_product(r, b, w, (p_own, p_x), y, gal, 1)


def outer_kernel(w, span, gal, y, far_s, out):
    own = y.shape[1] - 2 * span
    by_s = dot(y[:, own : own + span], far_s[...])
    out[:, :w] = by_s[:, 2 * w :].astype(BF16)
    out[:, w : 2 * w] = (gal[:, :w] + by_s[:, w : 2 * w]).astype(BF16)
    out[:, 2 * w : 3 * w] = (gal[:, w : 2 * w] + by_s[:, :w]).astype(BF16)
    out[:, 3 * w : 4 * w] = gal[:, 2 * w :].astype(BF16)
    out[:, 4 * w :] = y[:, own + span :]


def flip(r, b, p, flipped):
    for j in range(r):
        at = slice(j * b, (j + 1) * b)
        flipped[:, at] = p[at, :].T


def left_product(r, b, dense, p, y, flipped):
    flip(r, b, p, flipped)
    y[...] = dot(flipped[...], dense[...]).astype(BF16)


def right_product(r, b, w, parts, y, gal, first=0):
    for d, other in enumerate(parts, first):
        gal[:, d * w : (d + 1) * w] = dot(y[:, : r * b], other[...])


def rest_kernel(which, r, b, w, dense, p_s, p_own, p_x, y, gal, flipped):
    parts = (p_s, p_own, p_x)
    left_product(r, b, dense, parts[which], y, flipped)
    right_product(r, b, w, parts, y, gal)


def galerkin_rows(w, span, gal, y, far_s, far_x):
    own = y.shape[1] - 2 * span
    by_s = dot(y[:, own : own + span], far_s[...])
    by_x = dot(y[:, own + span :], far_x[...])
    return (
        by_s[:, 2 * w :],
        gal[:, :w] + by_s[:, w : 2 * w],
        gal[:, w : 2 * w] + by_s[:, :w] + by_x[:, 2 * w :],
        gal[:, 2 * w :] + by_x[:, w : 2 * w],
        by_x[:, :w],
    )


def chip_kernel(w, span, gal, y, far_s, far_x, out):
    for c, value in enumerate(galerkin_rows(w, span, gal, y, far_s, far_x)):
        out[:, c * w : (c + 1) * w] = value.astype(BF16)


def inner_kernel(w, span, gal, y, far_s, far_x, from_s, out):
    mine = galerkin_rows(w, span, gal, y, far_s, far_x)
    for u in range(-3, 4):
        total = mine[2 - u] if abs(u) < 3 else jnp.zeros((w, w), F32)
        if 0 <= 1 + u < 5:
            total = total + from_s[:, (1 + u) * w : (2 + u) * w].astype(F32)
        out[:, (3 - u) * w : (4 - u) * w] = total


def final_kernel(w, index, mine, sent_x, from_x, out_hbm, out, sems):
    sign = 1 - 2 * (index[0] & 1)
    back = dot(from_x[:, 4 * w :], sent_x[...])
    copies = []
    for u in (3, 2, -3, -2, -1, 0, 1):
        total = mine[:, (3 - u) * w : (4 - u) * w]
        if 0 <= 3 + u < 4:
            total = total + from_x[:, (3 + u) * w : (4 + u) * w].astype(F32)
        if abs(u) < 2:
            total = total + back[:, (1 - u) * w : (2 - u) * w]
        out[u + 3, :, :] = total.astype(BF16)
        copies.append(pltpu.make_async_copy(out.at[u + 3], out_hbm.at[:, rows(3 + sign * u, w)], sems.at[u + 3]))
        copies[-1].start()
    for copy in copies:
        copy.wait()


def swap(x, route):
    return lax.ppermute(x, AXES, route)


def shards(block_values, block_columns, tentative, inverse_diagonal, aggregate, ghost_rows, damping):
    r, k = block_columns.shape
    b = tentative.shape[1]
    s = ghost_rows.shape[2]
    w = CA * b
    span = s * b
    devices = lax.axis_size(AXES)
    chip = [(i, i ^ 1) for i in range(devices) if i ^ 1 < devices]
    cross = []
    for i in range(1, devices - 1, 2):
        cross += [(i, i + 1), (i + 1, i)]
    index = lax.axis_index(AXES).astype(jnp.int32).reshape(1)
    group = lax.axis_size(AXES[1])
    tent = tentative.reshape(r * b, b)
    inv = inverse_diagonal.reshape(r * b, b)
    dma = pltpu.SemaphoreType.DMA
    total = (r + 2 * s) * b

    (pay,) = call(
        functools.partial(pack_kernel, r, b, s), (aggregate, ghost_rows, tent), "hhh",
        [((r * b + META, b), BF16)],
        scratch=[SMEM((r,), jnp.int32), SMEM((1, 2, s), jnp.int32), dma((3,))], limit=2 << 20,
    )
    pay_x = swap(pay, cross)
    pay_s = swap(pay, chip)
    dense, inv, p_own, damp = call(
        functools.partial(own_kernel, r, k, b, s),
        (index, damping, aggregate, block_columns, inv, block_values, pay), "sshhhhv",
        [((r * b, total), BF16), ((r * b, b), BF16), ((r * b, w), BF16), ((8, w), F32)],
        scratch=[
            SMEM((r,), jnp.int32), SMEM((r, k), jnp.int32), VMEM((r, k, b, b), BF16),
            VMEM((r * b, w), BF16), VMEM((r * b, w), BF16), dma((r + 3,)),
        ],
        flops=2 * r * b * r * b * w, limit=24 << 20,
    )
    (p_s,) = call(
        functools.partial(near_kernel, r, b, s), (ghost_rows, index, damp, dense, inv, pay_s), "vsvvvv",
        [((r * b, w), BF16)], scratch=[VMEM((META, b), F32), VMEM((span, w), BF16), VMEM((r * b, w), BF16)],
        flops=2 * r * b * span * w, limit=24 << 20,
    )
    p_x, out_x, out_s = call(
        functools.partial(far_kernel, r, b, s, w),
        (ghost_rows, index, damp, dense, inv, p_s, p_own, pay_s, pay_x), "vsvvvvvvv",
        [((r * b, w), BF16), ((span, 3 * w), BF16), ((span, 3 * w), BF16)],
        scratch=[VMEM((META, b), F32), VMEM((META, b), F32), VMEM((span, w), BF16), VMEM((r * b, w), BF16)],
        flops=2 * r * b * span * w, limit=24 << 20,
    )
    far_x = swap(out_x, cross)
    far_s = swap(out_s, chip)
    shapes = [((w, total), BF16), ((w, 3 * w), F32)]
    scratch = [VMEM((w, r * b), BF16)]
    flops = 2 * r * b * r * b * 2 * w
    y_x, gal_x = call(
        functools.partial(ahead_kernel, group, r, b, w), (index, dense, p_s, p_x), "svvv",
        shapes, scratch=scratch, flops=flops, limit=24 << 20,
    )
    y_x, gal_x = call(
        functools.partial(cross_kernel, group, r, b, w), (index, dense, p_s, p_own, p_x, y_x, gal_x), "svvvvvv",
        shapes, scratch=scratch, flops=flops, limit=24 << 20, aliases={5: 0, 6: 1},
    )
    (sum_x,) = call(
        functools.partial(outer_kernel, w, span), (gal_x, y_x, far_s), "vvv",
        [((w, 4 * w + span), BF16)], flops=2 * w * span * 3 * w, limit=16 << 20,
    )
    from_x = swap(sum_x, cross)

    def rest(which):
        return call(
            functools.partial(rest_kernel, which, r, b, w), (dense, p_s, p_own, p_x), "vvvv",
            shapes, scratch=scratch, flops=flops, limit=24 << 20,
        )

    y_s, gal_s = rest(0)
    (sum_s,) = call(
        functools.partial(chip_kernel, w, span), (gal_s, y_s, far_s, far_x), "vvvv",
        [((w, 5 * w), BF16)], flops=4 * w * span * 3 * w, limit=16 << 20,
    )
    from_s = swap(sum_s, chip)
    y_own, gal_own = rest(1)
    (mine,) = call(
        functools.partial(inner_kernel, w, span), (gal_own, y_own, far_s, far_x, from_s), "vvvvv",
        [((w, 7 * w), F32)], flops=4 * w * span * 3 * w, limit=16 << 20,
    )
    (out,) = call(
        functools.partial(final_kernel, w), (index, mine, out_x, from_x), "svvv",
        [((w, 7 * w), BF16)], scratch=[VMEM((7, w, w), BF16), dma((7,))],
        flops=2 * w * span * 3 * w, limit=16 << 20, out_space=pltpu.HBM,
    )
    return out.reshape(CA, b, 7 * w)


def solution(mesh):
    return jax.shard_map(
        shards,
        mesh=mesh,
        in_specs=(
            P(AXES, None, None, None),
            P(AXES, None),
            P(AXES, None, None),
            P(AXES, None, None),
            P(AXES),
            P(AXES, None, None),
            P(),
        ),
        out_specs=P(AXES, None, None),
        check_vma=False,
    )
```
